256 devices in a mesh: section: 4 (over x_hi, core), expert: 64 (over x_lo, z, y).
Axes of the slice: x: 4 (x_hi: 2, x_lo: 2; x = x_hi * 2 + x_lo), y: 4, z: 8, core: 2. Of those that a mesh axis runs over, the one named last changes fastest.
Arguments:
- x_fwd: bfloat16 [4, 8192, 3584], P('section', 'expert'), may hold values from -6 to 6
- routes_fwd: int32 [4, 8192, 2], P('section', 'expert'), may hold values from 0 to 31, all different within a row; in each aligned block of 128 rows (0 to 127, 128 to 255, ..., all dimensions but the last counted through in order) at most 12 rows name the same one
- affinity_fwd: float32 [4, 8192, 2], P('section', 'expert'), may hold values from 0.1 to 1
- x_bwd: bfloat16 [4, 8192, 3584], P('section', 'expert'), may hold values from -6 to 6
- grad_bwd: bfloat16 [4, 8192, 3584], P('section', 'expert'), may hold values from -6 to 6
- routes_bwd: int32 [4, 8192, 2], P('section', 'expert'), may hold values from 0 to 31, all different within a row; in each aligned block of 128 rows (0 to 127, 128 to 255, ..., all dimensions but the last counted through in order) at most 12 rows name the same one
- affinity_bwd: float32 [4, 8192, 2], P('section', 'expert'), may hold values from 0.1 to 1
- up_weight: bfloat16 [4, 3584, 32768], P('section', None, 'expert'), may hold values from -0.09375 to 0.09375
- down_weight: bfloat16 [4, 32768, 3584], P('section', 'expert'), may hold values from -0.1875 to 0.1875
Outputs:
- fwd_next: bfloat16 [4, 8192, 3584], P('section', 'expert')
- bwd_next: bfloat16 [4, 8192, 3584], P('section', 'expert')
The draws below stay inside these ranges and needn't reach their ends.
Inputs may be any that keep to these rules, and one draw needn't show every extreme that they name: `routes_fwd`: each row names 2 different experts; in each section, among the 128 rows of one device (aligned blocks), no expert is named more than 12 times, a bound that some block reaches. `routes_bwd`: each row names 2 different experts; in each section, among the 128 rows of one device (aligned blocks), no expert is named more than 12 times, a bound that some block reaches.
All inputs are finite; a program needn't handle non-finite values.
Results may differ from the reference program's by a relative error of at most 0.0041.
Values may be sent and summed in bfloat16 or wider, within the bound.
No kernel may reach another device: no remote copies, remote signals or barrier semaphores. Data moves between devices by JAX's collectives and lax.ppermute only.
A program may use at most 128 MiB of HBM per device.

```python
import math
import jax
import jax.numpy as jnp
import numpy as np
from jax import lax

D = 3584
HID = 1024
TOP = 2
TOK_DEV = 128
SECTIONS = 4
EXPERTS = 32
TOKENS = 8192
CAP = 12
N_EXPERT = 64


def steps_of(key, shape, split, least, high):
    level, own = 1.0, jax.random.fold_in(key, 6)
    for position, shards_of in split:
        steps = jnp.exp(jax.random.uniform(jax.random.fold_in(own, position), (shards_of,), jnp.float32, least / len(split), high / len(split)))
        level = level * jnp.repeat(steps, shape[position] // shards_of).reshape([-1 if axis == position else 1 for axis in range(len(shape))])
    return level


def assign_block(stream_key, own, number, rows, count, top, limit, lean):
    sequence = jax.random.permutation(stream_key, count)
    crowded, ordinary = portions_of(count, rows * top, limit, lean, True), portions_of(count, rows * top, limit, lean, False)
    places = jnp.arange(count)

    def named(tallies, rotation):
        used = int((tallies > 0).sum())
        fixed = max(1, used // 4)
        passed = fixed + (places - fixed + rotation * (used - fixed)) % max(1, count - fixed)
        return jnp.zeros((count,), jnp.int32).at[sequence[jnp.where(places < fixed, places, passed)]].set(jnp.asarray(tallies, jnp.int32))

    tallies = jnp.where(number % 4 == 0, named(crowded, number // 4), named(ordinary, number - number // 4 - 1))
    mixed = jax.random.permutation(jax.random.fold_in(own, 3), count)
    giver, sink = mixed[0:count // 2 * 2:2], mixed[1:count // 2 * 2:2]
    slack = jnp.minimum(tallies[giver] - 1, limit - tallies[sink]) // 2
    slack = jnp.where((giver == sequence[0]) | (sink == sequence[0]) | (tallies[sink] == 0), 0, jnp.maximum(slack, 0))
    passed = jax.random.randint(jax.random.fold_in(own, 4), (count // 2,), 0, 1 << 20) % (slack + 1)
    tallies = tallies.at[giver].add(-passed).at[sink].add(passed)
    labels = jnp.searchsorted(jnp.cumsum(tallies), jnp.arange(rows * top), side="right").astype(jnp.int32)
    listing = labels.reshape(top, rows).T
    listing = listing[jax.random.permutation(jax.random.fold_in(own, 1), rows)]
    rotation = jax.random.randint(jax.random.fold_in(own, 2), (rows, 1), 0, top)
    return jnp.take_along_axis(listing, (jnp.arange(top)[None, :] + rotation) % top, axis=1)


def portions_of(count, total, limit, skew, full):
    portions = [(1 << 20) // math.isqrt(standing ** skew) + 1 for standing in range(1, count + 1)]
    largest = limit if full else min(limit, max(-(-total // count), total * portions[0] // sum(portions)))
    least = 1 if total - largest >= count - 1 else 0
    holding, surplus = [largest] + [least] * (count - 1), total - largest - least * (count - 1)
    while surplus > 0:
        free = [i for i in range(1, count) if holding[i] < largest] or [i for i in range(1, count) if holding[i] < limit]
        whole, left = sum([portions[i] for i in free]), surplus
        for i in free:
            extra = min(limit - holding[i], max(1, left * portions[i] // whole), surplus)
            holding[i] = holding[i] + extra
            surplus = surplus - extra
    return np.array(holding)


def gaussian(key, dims, deviation, bound, split=(), kind=jnp.bfloat16):
    array = deviation * jax.random.normal(key, dims, jnp.float32)
    if split:
        array = array * steps_of(key, dims, split, -0.22, 0.18)
    return jnp.clip(array, -bound, bound).astype(kind)


def setup_inputs(seed: int = 0) -> dict:
    keys = jax.random.split(jax.random.key(seed), 10)
    x_fwd = gaussian(keys[0], (SECTIONS, TOKENS, D), 1.0, 6.0, ((0, 4), (1, 64)))
    routes_fwd_keys = jax.random.split(jax.random.fold_in(keys[1], 1), SECTIONS * TOKENS // TOK_DEV)
    routes_fwd_turns = jax.random.permutation(jax.random.fold_in(keys[1], 3), SECTIONS * TOKENS // TOK_DEV)
    routes_fwd = jax.vmap(lambda own, number: assign_block(jax.random.fold_in(keys[1], 2), own, number, TOK_DEV, EXPERTS, TOP, CAP, 2))(routes_fwd_keys, routes_fwd_turns).reshape((SECTIONS, TOKENS, TOP))
    affinity_fwd = jnp.clip(jnp.exp(math.log(1.0) - 2.3025851 * jax.random.uniform(keys[2], (SECTIONS, TOKENS, TOP), jnp.float32) ** steps_of(keys[2], (SECTIONS, TOKENS, TOP), ((0, 4), (1, 64)), -0.2, 0.2)), 0.1, 1.0)
    x_bwd = gaussian(keys[3], (SECTIONS, TOKENS, D), 1.0, 6.0, ((0, 4), (1, 64)))
    grad_bwd = gaussian(keys[4], (SECTIONS, TOKENS, D), 1.0, 6.0, ((0, 4), (1, 64)))
    routes_bwd_keys = jax.random.split(jax.random.fold_in(keys[5], 1), SECTIONS * TOKENS // TOK_DEV)
    routes_bwd_turns = jax.random.permutation(jax.random.fold_in(keys[5], 3), SECTIONS * TOKENS // TOK_DEV)
    routes_bwd = jax.vmap(lambda own, number: assign_block(jax.random.fold_in(keys[5], 2), own, number, TOK_DEV, EXPERTS, TOP, CAP, 2))(routes_bwd_keys, routes_bwd_turns).reshape((SECTIONS, TOKENS, TOP))
    affinity_bwd = jnp.clip(jnp.exp(math.log(1.0) - 2.3025851 * jax.random.uniform(keys[6], (SECTIONS, TOKENS, TOP), jnp.float32) ** steps_of(keys[6], (SECTIONS, TOKENS, TOP), ((0, 4), (1, 64)), -0.2, 0.2)), 0.1, 1.0)
    up_weight = gaussian(keys[7], (SECTIONS, D, EXPERTS * HID), D ** -0.5, 0.09375, ((0, 4), (2, 64)))
    down_weight = gaussian(keys[8], (SECTIONS, EXPERTS * HID, D), HID ** -0.5, 0.1875, ((0, 4), (1, 64)))
    return {"x_fwd": x_fwd, "routes_fwd": routes_fwd, "affinity_fwd": affinity_fwd, "x_bwd": x_bwd, "grad_bwd": grad_bwd, "routes_bwd": routes_bwd, "affinity_bwd": affinity_bwd, "up_weight": up_weight, "down_weight": down_weight}


def silu_grad(values):
    sigma = jax.nn.sigmoid(values)
    return sigma * (1.0 + values * (1.0 - sigma))

def expert_pass(rows_fwd, rows_saved, rows_grad, up_block, down_block):
    half_count = HID // 2
    sums_fwd = jnp.zeros((rows_fwd.shape[0], D), jnp.float32)
    sums_bwd = jnp.zeros((rows_fwd.shape[0], D), jnp.float32)
    for half_id in range(2):
        up_part = up_block[:, half_id * half_count:(half_id + 1) * half_count]
        down_part = down_block[half_id * half_count:(half_id + 1) * half_count, :]
        hidden = jax.nn.silu(jnp.dot(rows_fwd, up_part, preferred_element_type=jnp.float32)).astype(jnp.bfloat16)
        part_fwd = jnp.dot(hidden, down_part, preferred_element_type=jnp.float32).astype(jnp.bfloat16)
        pre_act = jnp.dot(rows_saved, up_part, preferred_element_type=jnp.float32)
        hidden_grad = jnp.dot(rows_grad, down_part.T, preferred_element_type=jnp.float32)
        pre_grad = (hidden_grad * silu_grad(pre_act)).astype(jnp.bfloat16)
        part_bwd = jnp.dot(pre_grad, up_part.T, preferred_element_type=jnp.float32).astype(jnp.bfloat16)
        sums_fwd = sums_fwd + part_fwd.astype(jnp.float32)
        sums_bwd = sums_bwd + part_bwd.astype(jnp.float32)
    return (sums_fwd.astype(jnp.bfloat16), sums_bwd.astype(jnp.bfloat16))

def combine(inputs, results, affinity):
    weights = affinity / lax.optimization_barrier(jnp.sum(affinity, -1, keepdims=True))
    routed = results.reshape(TOKENS, TOP, D).astype(jnp.float32)
    return (inputs.astype(jnp.float32) + lax.optimization_barrier(jnp.sum(weights[..., None] * routed, 1))).astype(jnp.bfloat16)

def reference(x_fwd, routes_fwd, affinity_fwd, x_bwd, grad_bwd, routes_bwd, affinity_bwd, up_weight, down_weight):
    total = TOKENS * TOP
    rows = N_EXPERT * CAP
    zero_row = jnp.zeros((1, D), jnp.bfloat16)
    layer_outs = []
    input_grads = []
    for section_id in range(SECTIONS):
        inputs_fwd = jnp.concatenate([x_fwd[section_id], zero_row], 0)
        inputs_saved = jnp.concatenate([x_bwd[section_id], zero_row], 0)
        inputs_grad = jnp.concatenate([grad_bwd[section_id], zero_row], 0)
        flat_fwd = routes_fwd[section_id].reshape(-1)
        flat_bwd = routes_bwd[section_id].reshape(-1)
        up_section = up_weight[section_id]
        down_section = down_weight[section_id]

        def one_expert(carry, expert_id):
            results_fwd, results_bwd = carry
            index_fwd = jnp.nonzero(flat_fwd == expert_id, size=rows, fill_value=total)[0].astype(jnp.int32)
            index_bwd = jnp.nonzero(flat_bwd == expert_id, size=rows, fill_value=total)[0].astype(jnp.int32)
            up_block = lax.dynamic_slice_in_dim(up_section, (expert_id * HID).astype(jnp.int32), HID, 1)
            down_block = lax.dynamic_slice_in_dim(down_section, (expert_id * HID).astype(jnp.int32), HID, 0)
            token_fwd = index_fwd // TOP
            token_bwd = index_bwd // TOP
            outs_fwd, outs_bwd = expert_pass(inputs_fwd[token_fwd], inputs_saved[token_bwd], inputs_grad[token_bwd], up_block, down_block)
            results_fwd = results_fwd.at[index_fwd].set(outs_fwd)
            results_bwd = results_bwd.at[index_bwd].set(outs_bwd)
            return ((results_fwd, results_bwd), None)
        start = jnp.zeros((total + 1, D), jnp.bfloat16)
        (results_fwd, results_bwd), _ = lax.scan(one_expert, (start, start), jnp.arange(EXPERTS, dtype=jnp.int32))
        layer_outs.append(combine(x_fwd[section_id], results_fwd[:total], affinity_fwd[section_id]))
        input_grads.append(combine(grad_bwd[section_id], results_bwd[:total], affinity_bwd[section_id]))
    layer_out = jnp.stack(layer_outs)
    input_grad = jnp.stack(input_grads)
    return (jnp.roll(layer_out, 1, 0), jnp.roll(input_grad, -1, 0))
```

```python
import functools

import jax
import jax.numpy as jnp
from jax import lax
from jax.experimental import pallas as pl
from jax.experimental.pallas import tpu as pltpu
from jax.sharding import PartitionSpec as P

VMEM = pl.BlockSpec(memory_space=pltpu.VMEM)


def same_side_groups(devices):
    sides = [0 if d % 4 in (0, 3) else 1 for d in range(devices)]
    return [[d for d in range(devices) if sides[d] == side] for side in (0, 1)]


def from_partner(block, axis):
    count = lax.axis_size(axis)
    return lax.ppermute(block, axis, [(i, i ^ 1) for i in range(count)])


def shifted(shard, axis, by):
    size = lax.axis_size(axis)
    return lax.ppermute(shard, axis, [(i, (i + by) % size) for i in range(size)])


def silu_grad(values):
    sigma = jax.nn.sigmoid(values)
    return sigma * (1.0 + values * (1.0 - sigma))


def place_of(routes, experts):
    tokens = routes.shape[1]
    expert_id = lax.broadcasted_iota(jnp.int32, (experts, tokens), 0)
    named = (expert_id == routes[0:1, :]) | (expert_id == routes[1:2, :])
    earlier = (
        lax.broadcasted_iota(jnp.int32, (tokens, tokens), 0)
        < lax.broadcasted_iota(jnp.int32, (tokens, tokens), 1)
    )
    before = jnp.dot(
        named.astype(jnp.float32).astype(jnp.bfloat16),
        earlier.astype(jnp.float32).astype(jnp.bfloat16),
        preferred_element_type=jnp.float32,
    )
    return jnp.where(named, before, -1.0)


def slot_rows(place, block, first, capacity):
    experts, tokens = place.shape
    rows = experts * block
    row = lax.broadcasted_iota(jnp.int32, (rows, experts), 0)
    col = lax.broadcasted_iota(jnp.int32, (rows, experts), 1)
    begin = col * block + first
    mine = (row >= begin) & (row < begin + capacity)
    spread = mine.astype(jnp.float32).astype(jnp.bfloat16)
    within = jnp.sum(jnp.where(mine, row - begin + 1, 0).astype(jnp.float32), 1, keepdims=True) - 1.0
    slot = jnp.dot(
        spread, (place + 1.0).astype(jnp.bfloat16), preferred_element_type=jnp.float32
    ) - 1.0
    return (slot == within) & (within >= 0.0)


def as_bf16(mask):
    return mask.astype(jnp.float32).astype(jnp.bfloat16)


def dispatch_fwd_kernel(capacity, experts, routes_ref, x_ref, out_ref):
    place = place_of(routes_ref[...], experts)
    pick = as_bf16(slot_rows(place, capacity, 0, capacity))
    rows = jnp.dot(pick, x_ref[...], preferred_element_type=jnp.float32)
    out_ref[...] = rows.reshape(out_ref.shape).astype(jnp.bfloat16)


def dispatch_bwd_kernel(capacity, experts, routes_ref, x_ref, g_ref, out_ref):
    place = place_of(routes_ref[...], experts)
    pick_x = as_bf16(slot_rows(place, 2 * capacity, 0, capacity))
    pick_g = as_bf16(slot_rows(place, 2 * capacity, capacity, capacity))
    rows = jnp.dot(pick_x, x_ref[...], preferred_element_type=jnp.float32)
    rows = rows + jnp.dot(pick_g, g_ref[...], preferred_element_type=jnp.float32)
    out_ref[...] = rows.astype(jnp.bfloat16)


def combine_kernel(capacity, experts, routes_ref, affinity_ref, x_ref, back_ref, out_ref):
    routes = routes_ref[...]
    affinity = affinity_ref[...]
    tokens = routes.shape[1]
    rows = experts * capacity
    pick = slot_rows(place_of(routes, experts), capacity, 0, capacity)
    row = lax.broadcasted_iota(jnp.int32, (rows, tokens), 0)
    weights = affinity / jnp.sum(affinity, 0, keepdims=True)
    back = back_ref[...].reshape(rows, x_ref.shape[1])
    total = x_ref[...].astype(jnp.float32)
    for k in range(2):
        begin = routes[k : k + 1, :] * capacity
        mine = pick & (row >= begin) & (row < begin + capacity)
        picked = lax.dot_general(
            as_bf16(mine), back, (((0,), (0,)), ((), ())), preferred_element_type=jnp.float32
        )
        weight = jnp.broadcast_to(weights[k : k + 1, :], (tokens, tokens)).T[:, 0:1]
        total = total + weight * picked
    out_ref[...] = total.astype(jnp.bfloat16)


def per_device(
    x_fwd,
    routes_fwd,
    affinity_fwd,
    x_bwd,
    grad_bwd,
    routes_bwd,
    affinity_bwd,
    up_weight,
    down_weight,
):
    devices = lax.axis_size("expert")
    experts = devices // 2
    tokens = x_fwd.shape[1]
    model_width = x_fwd.shape[2]
    top_count = routes_fwd.shape[2]
    capacity = 3 * tokens * top_count // devices
    rows = experts * capacity
    groups = same_side_groups(devices)
    params = pltpu.CompilerParams(vmem_limit_bytes=60 * 1024 * 1024)

    up_own = up_weight[0]
    down_own = down_weight[0]
    up_other = from_partner(up_own, "expert")
    down_other = from_partner(down_own, "expert")

    routes_f = routes_fwd[0].T
    routes_b = routes_bwd[0].T

    def exchange(block):
        return lax.all_to_all(
            block, "expert", split_axis=0, concat_axis=0, tiled=True, axis_index_groups=groups
        )

    send_f = pl.pallas_call(
        functools.partial(dispatch_fwd_kernel, capacity, experts),
        out_shape=jax.ShapeDtypeStruct((rows // 4, 4, model_width), jnp.bfloat16),
        in_specs=[VMEM] * 2,
        out_specs=VMEM,
        compiler_params=params,
        name="dispatch_fwd",
    )(routes_f, x_fwd[0])
    recv_f = exchange(send_f)
    send_b = pl.pallas_call(
        functools.partial(dispatch_bwd_kernel, capacity, experts),
        out_shape=jax.ShapeDtypeStruct((2 * rows, model_width), jnp.bfloat16),
        in_specs=[VMEM] * 3,
        out_specs=VMEM,
        compiler_params=params,
        name="dispatch_bwd",
    )(routes_b, x_bwd[0], grad_bwd[0])
    recv_b = exchange(send_b)

    f32 = jnp.float32
    against_rows = (((1,), (1,)), ((), ()))

    x_rows = recv_f.reshape(rows, model_width)
    part = None
    for up, down in ((up_own, down_own), (up_other, down_other)):
        hidden = jax.nn.silu(jnp.dot(x_rows, up, preferred_element_type=f32)).astype(jnp.bfloat16)
        product = jnp.dot(hidden, down, preferred_element_type=f32)
        part = product if part is None else part + product
    back_f = exchange(part.astype(jnp.bfloat16).reshape(rows // 4, 4, model_width))

    blocks = recv_b.reshape(experts, 2 * capacity, model_width)
    x_rows = blocks[:, :capacity].reshape(rows, model_width)
    g_rows = blocks[:, capacity:].reshape(rows, model_width)
    part = None
    for up, down in ((up_own, down_own), (up_other, down_other)):
        pre_act = jnp.dot(x_rows, up, preferred_element_type=f32)
        hidden_grad = lax.dot_general(g_rows, down, against_rows, preferred_element_type=f32)
        pre_grad = (hidden_grad * silu_grad(pre_act)).astype(jnp.bfloat16)
        product = lax.dot_general(pre_grad, up, against_rows, preferred_element_type=f32)
        part = product if part is None else part + product
    back_b = exchange(part.astype(jnp.bfloat16).reshape(rows // 4, 4, model_width))

    def combine(routes, affinity, x, back, name):
        return pl.pallas_call(
            functools.partial(combine_kernel, capacity, experts),
            out_shape=jax.ShapeDtypeStruct((tokens, model_width), jnp.bfloat16),
            in_specs=[VMEM] * 4,
            out_specs=VMEM,
            compiler_params=params,
            name=name,
        )(routes, affinity, x, back)

    layer_out = combine(routes_f, affinity_fwd[0].T, x_fwd[0], back_f, "combine_fwd")
    fwd_next = shifted(layer_out[None], "section", 1)
    input_grad = combine(routes_b, affinity_bwd[0].T, grad_bwd[0], back_b, "combine_bwd")
    bwd_next = shifted(input_grad[None], "section", -1)
    return (fwd_next, bwd_next)


def solution(mesh):
    rows = P("section", "expert", None)
    in_specs = (rows,) * 7 + (P("section", None, "expert"), rows)
    return jax.shard_map(
        per_device, mesh=mesh, in_specs=in_specs, out_specs=(rows, rows), check_vma=False
    )
```

```python
import functools

import jax
import jax.numpy as jnp
from jax import lax
from jax.experimental import pallas as pl
from jax.experimental.pallas import tpu as pltpu
from jax.sharding import PartitionSpec as P


VMEM = pl.BlockSpec(memory_space=pltpu.VMEM)


def same_side_groups(devices):
    sides = [0 if d % 4 in (0, 3) else 1 for d in range(devices)]
    return [[d for d in range(devices) if sides[d] == side] for side in (0, 1)]


def from_partner(block, axis):
    count = lax.axis_size(axis)
    return lax.ppermute(block, axis, [(i, i ^ 1) for i in range(count)])


def shifted(shard, axis, by):
    size = lax.axis_size(axis)
    return lax.ppermute(shard, axis, [(i, (i + by) % size) for i in range(size)])


def silu_grad(values):
    sigma = jax.nn.sigmoid(values)
    return sigma * (1.0 + values * (1.0 - sigma))


def place_of(routes, experts):
    tokens = routes.shape[1]
    expert_id = lax.broadcasted_iota(jnp.int32, (experts, tokens), 0)
    named = (expert_id == routes[0:1, :]) | (expert_id == routes[1:2, :])
    earlier = (
        lax.broadcasted_iota(jnp.int32, (tokens, tokens), 0)
        < lax.broadcasted_iota(jnp.int32, (tokens, tokens), 1)
    )
    before = jnp.dot(
        named.astype(jnp.float32).astype(jnp.bfloat16),
        earlier.astype(jnp.float32).astype(jnp.bfloat16),
        preferred_element_type=jnp.float32,
    )
    return jnp.where(named, before, -1.0)


def slot_rows(place, block, first, capacity):
    experts, _ = place.shape
    rows = experts * block
    row = lax.broadcasted_iota(jnp.int32, (rows, experts), 0)
    col = lax.broadcasted_iota(jnp.int32, (rows, experts), 1)
    begin = col * block + first
    mine = (row >= begin) & (row < begin + capacity)
    spread = mine.astype(jnp.float32).astype(jnp.bfloat16)
    within = jnp.sum(jnp.where(mine, row - begin + 1, 0).astype(jnp.float32), 1, keepdims=True) - 1.0
    slot = jnp.dot(
        spread, (place + 1.0).astype(jnp.bfloat16), preferred_element_type=jnp.float32
    ) - 1.0
    return (slot == within) & (within >= 0.0)


def as_bf16(mask):
    return mask.astype(jnp.float32).astype(jnp.bfloat16)


def dispatch_fwd_kernel(capacity, experts, routes_ref, x_ref, out_ref):
    place = place_of(routes_ref[...], experts)
    pick = as_bf16(slot_rows(place, capacity, 0, capacity))
    rows = jnp.dot(pick, x_ref[...], preferred_element_type=jnp.float32)
    out_ref[...] = rows.reshape(out_ref.shape).astype(jnp.bfloat16)


def dispatch_bwd_kernel(capacity, experts, routes_ref, x_ref, g_ref, out_ref):
    place = place_of(routes_ref[...], experts)
    pick_x = as_bf16(slot_rows(place, 2 * capacity, 0, capacity))
    pick_g = as_bf16(slot_rows(place, 2 * capacity, capacity, capacity))
    rows = jnp.dot(pick_x, x_ref[...], preferred_element_type=jnp.float32)
    rows = rows + jnp.dot(pick_g, g_ref[...], preferred_element_type=jnp.float32)
    out_ref[...] = rows.astype(jnp.bfloat16)


def combine_kernel(capacity, experts, routes_ref, affinity_ref, x_ref, back_ref, out_ref):
    routes = routes_ref[...]
    affinity = affinity_ref[...]
    tokens = routes.shape[1]
    rows = experts * capacity
    pick = slot_rows(place_of(routes, experts), capacity, 0, capacity)
    row = lax.broadcasted_iota(jnp.int32, (rows, tokens), 0)
    weights = affinity / jnp.sum(affinity, 0, keepdims=True)
    back = back_ref[...].reshape(rows, x_ref.shape[1])
    total = x_ref[...].astype(jnp.float32)
    for k in range(2):
        begin = routes[k : k + 1, :] * capacity
        mine = pick & (row >= begin) & (row < begin + capacity)
        picked = lax.dot_general(
            as_bf16(mine), back, (((0,), (0,)), ((), ())), preferred_element_type=jnp.float32
        )
        weight = jnp.broadcast_to(weights[k : k + 1, :], (tokens, tokens)).T[:, 0:1]
        total = total + weight * picked
    out_ref[...] = total.astype(jnp.bfloat16)


def layer(
    x_fwd,
    routes_fwd,
    affinity_fwd,
    x_bwd,
    grad_bwd,
    routes_bwd,
    affinity_bwd,
    up_weight,
    down_weight,
):
    devices = lax.axis_size("expert")
    experts = devices // 2
    tokens = x_fwd.shape[1]
    model_width = x_fwd.shape[2]
    top_count = routes_fwd.shape[2]
    capacity = 3 * tokens * top_count // devices
    rows = experts * capacity
    groups = same_side_groups(devices)
    params = pltpu.CompilerParams(vmem_limit_bytes=60 * 1024 * 1024)

    up_own = up_weight[0]
    down_own = down_weight[0]
    up_other = from_partner(up_own, "expert")
    down_other = from_partner(down_own, "expert")

    routes_f = routes_fwd[0].T
    routes_b = routes_bwd[0].T

    def exchange(block):
        return lax.all_to_all(
            block, "expert", split_axis=0, concat_axis=0, tiled=True, axis_index_groups=groups
        )

    send_f = pl.pallas_call(
        functools.partial(dispatch_fwd_kernel, capacity, experts),
        out_shape=jax.ShapeDtypeStruct((rows // 4, 4, model_width), jnp.bfloat16),
        in_specs=[VMEM] * 2,
        out_specs=VMEM,
        compiler_params=params,
        name="dispatch_fwd",
    )(routes_f, x_fwd[0])
    recv_f = exchange(send_f)
    send_b = pl.pallas_call(
        functools.partial(dispatch_bwd_kernel, capacity, experts),
        out_shape=jax.ShapeDtypeStruct((2 * rows, model_width), jnp.bfloat16),
        in_specs=[VMEM] * 3,
        out_specs=VMEM,
        compiler_params=params,
        name="dispatch_bwd",
    )(routes_b, x_bwd[0], grad_bwd[0])
    recv_b = exchange(send_b)

    f32 = jnp.float32
    against_rows = (((1,), (1,)), ((), ()))

    x_rows = recv_f.reshape(rows, model_width)
    part = None
    for up, down in ((up_own, down_own), (up_other, down_other)):
        hidden = jax.nn.silu(jnp.dot(x_rows, up, preferred_element_type=f32)).astype(jnp.bfloat16)
        product = jnp.dot(hidden, down, preferred_element_type=f32)
        part = product if part is None else part + product
    back_f = exchange(part.astype(jnp.bfloat16).reshape(rows // 4, 4, model_width))

    blocks = recv_b.reshape(experts, 2 * capacity, model_width)
    x_rows = blocks[:, :capacity].reshape(rows, model_width)
    g_rows = blocks[:, capacity:].reshape(rows, model_width)
    part = None
    for up, down in ((up_own, down_own), (up_other, down_other)):
        pre_act = jnp.dot(x_rows, up, preferred_element_type=f32)
        hidden_grad = lax.dot_general(g_rows, down, against_rows, preferred_element_type=f32)
        pre_grad = (hidden_grad * silu_grad(pre_act)).astype(jnp.bfloat16)
        product = lax.dot_general(pre_grad, up, against_rows, preferred_element_type=f32)
        part = product if part is None else part + product
    back_b = exchange(part.astype(jnp.bfloat16).reshape(rows // 4, 4, model_width))

    def combine(routes, affinity, x, back):
        return pl.pallas_call(
            functools.partial(combine_kernel, capacity, experts),
            out_shape=jax.ShapeDtypeStruct((tokens, model_width), jnp.bfloat16),
            in_specs=[VMEM] * 4,
            out_specs=VMEM,
            compiler_params=params,
        )(routes, affinity, x, back)

    layer_out = combine(routes_f, affinity_fwd[0].T, x_fwd[0], back_f)
    fwd_next = shifted(layer_out[None], "section", 1)
    input_grad = combine(routes_b, affinity_bwd[0].T, grad_bwd[0], back_b)
    bwd_next = shifted(input_grad[None], "section", -1)
    return (fwd_next, bwd_next)


def solution(mesh):
    rows = P("section", "expert", None)
    in_specs = (rows,) * 7 + (P("section", None, "expert"), rows)
    return jax.shard_map(
        layer, mesh=mesh, in_specs=in_specs, out_specs=(rows, rows), check_vma=False
    )
```

```python
import functools

import jax
import jax.numpy as jnp
from jax import lax
from jax.experimental import pallas as pl
from jax.experimental.pallas import tpu as pltpu
from jax.sharding import PartitionSpec as P


VMEM = pl.BlockSpec(memory_space=pltpu.VMEM)
ANY = pl.BlockSpec(memory_space=pl.ANY)
AGAINST_ROWS = (((1,), (1,)), ((), ()))
STEP = 512


def same_side_groups(devices):
    sides = [0 if d % 4 in (0, 3) else 1 for d in range(devices)]
    return [[d for d in range(devices) if sides[d] == side] for side in (0, 1)]


def from_partner(block, axis):
    count = lax.axis_size(axis)
    return lax.ppermute(block, axis, [(i, i ^ 1) for i in range(count)])


def shifted(shard, axis, by):
    size = lax.axis_size(axis)
    return lax.ppermute(shard, axis, [(i, (i + by) % size) for i in range(size)])


def silu_grad(values):
    sigma = jax.nn.sigmoid(values)
    return sigma * (1.0 + values * (1.0 - sigma))


def place_of(routes, experts):
    tokens = routes.shape[1]
    expert_id = lax.broadcasted_iota(jnp.int32, (experts, tokens), 0)
    named = (expert_id == routes[0:1, :]) | (expert_id == routes[1:2, :])
    earlier = (
        lax.broadcasted_iota(jnp.int32, (tokens, tokens), 0)
        < lax.broadcasted_iota(jnp.int32, (tokens, tokens), 1)
    )
    before = jnp.dot(
        named.astype(jnp.float32).astype(jnp.bfloat16),
        earlier.astype(jnp.float32).astype(jnp.bfloat16),
        preferred_element_type=jnp.float32,
    )
    return jnp.where(named, before, -1.0)


def slot_rows(place, block, first, capacity):
    experts, _ = place.shape
    rows = experts * block
    row = lax.broadcasted_iota(jnp.int32, (rows, experts), 0)
    col = lax.broadcasted_iota(jnp.int32, (rows, experts), 1)
    begin = col * block + first
    mine = (row >= begin) & (row < begin + capacity)
    spread = mine.astype(jnp.float32).astype(jnp.bfloat16)
    within = jnp.sum(jnp.where(mine, row - begin + 1, 0).astype(jnp.float32), 1, keepdims=True) - 1.0
    slot = jnp.dot(
        spread, (place + 1.0).astype(jnp.bfloat16), preferred_element_type=jnp.float32
    ) - 1.0
    return (slot == within) & (within >= 0.0)


def as_bf16(mask):
    return mask.astype(jnp.float32).astype(jnp.bfloat16)


def dispatch_fwd_kernel(capacity, experts, routes_ref, x_ref, out_ref):
    place = place_of(routes_ref[...], experts)
    pick = as_bf16(slot_rows(place, capacity, 0, capacity))
    rows = jnp.dot(pick, x_ref[...], preferred_element_type=jnp.float32)
    out_ref[...] = rows.reshape(out_ref.shape).astype(jnp.bfloat16)


def dispatch_bwd_kernel(capacity, experts, routes_ref, x_ref, g_ref, out_ref):
    place = place_of(routes_ref[...], experts)
    pick_x = as_bf16(slot_rows(place, 2 * capacity, 0, capacity))
    pick_g = as_bf16(slot_rows(place, 2 * capacity, capacity, capacity))
    rows = jnp.dot(pick_x, x_ref[...], preferred_element_type=jnp.float32)
    rows = rows + jnp.dot(pick_g, g_ref[...], preferred_element_type=jnp.float32)
    out_ref[...] = rows.reshape(out_ref.shape).astype(jnp.bfloat16)


def start_loads(up_own, down_own, up_other, down_other, ups, downs, sems):
    pairs = ((up_own, ups.at[0]), (down_own, downs.at[0]), (up_other, ups.at[1]), (down_other, downs.at[1]))
    loads = [pltpu.make_async_copy(src, dst, sems.at[i]) for i, (src, dst) in enumerate(pairs)]
    for load in loads:
        load.start()
    return loads


def expert_fwd_kernel(
    recv_ref, up_own, down_own, up_other, down_other, out_ref, ups, downs, hidden, sems
):
    groups, per_group, width = out_ref.shape
    rows = groups * per_group
    half = hidden.shape[1] // 2
    loads = start_loads(up_own, down_own, up_other, down_other, ups, downs, sems)
    x = recv_ref[...].reshape(rows, width)
    for i in range(2):
        loads[2 * i].wait()
        pre_act = jnp.dot(x, ups[i], preferred_element_type=jnp.float32)
        hidden[:, i * half : (i + 1) * half] = jax.nn.silu(pre_act).astype(jnp.bfloat16)
    loads[1].wait()
    loads[3].wait()
    for c in range(0, width, STEP):
        part = jnp.dot(
            hidden[:, :half], downs[0, :, c : c + STEP], preferred_element_type=jnp.float32
        )
        part = part + jnp.dot(
            hidden[:, half:], downs[1, :, c : c + STEP], preferred_element_type=jnp.float32
        )
        out_ref[:, :, c : c + STEP] = part.reshape(groups, per_group, STEP).astype(jnp.bfloat16)


def expert_bwd_kernel(
    recv_ref, up_own, down_own, up_other, down_other, out_ref, ups, downs, hidden, sems
):
    groups, per_group, width = out_ref.shape
    rows = groups * per_group
    half = hidden.shape[1] // 2
    loads = start_loads(up_own, down_own, up_other, down_other, ups, downs, sems)
    sources = hidden.shape[1] // 32
    both = recv_ref[...].reshape(sources, 2 * groups // sources, per_group, width)
    x = both[:, : groups // sources].reshape(rows, width)
    g = both[:, groups // sources :].reshape(rows, width)
    for i in range(2):
        loads[2 * i].wait()
        pre_act = jnp.dot(x, ups[i], preferred_element_type=jnp.float32)
        loads[2 * i + 1].wait()
        hidden_grad = lax.dot_general(
            g, downs[i], AGAINST_ROWS, preferred_element_type=jnp.float32
        )
        pre_grad = hidden_grad * silu_grad(pre_act)
        hidden[:, i * half : (i + 1) * half] = pre_grad.astype(jnp.bfloat16)
    for c in range(0, width, STEP):
        part = lax.dot_general(
            hidden[:, :half], ups[0, c : c + STEP, :], AGAINST_ROWS,
            preferred_element_type=jnp.float32,
        )
        part = part + lax.dot_general(
            hidden[:, half:], ups[1, c : c + STEP, :], AGAINST_ROWS,
            preferred_element_type=jnp.float32,
        )
        out_ref[:, :, c : c + STEP] = part.reshape(groups, per_group, STEP).astype(jnp.bfloat16)


def combine_kernel(capacity, experts, info_ref, x_ref, back_ref, out_ref):
    routes = info_ref[0:2, :].astype(jnp.int32)
    affinity = info_ref[2:4, :]
    tokens = routes.shape[1]
    rows = experts * capacity
    pick = slot_rows(place_of(routes, experts), capacity, 0, capacity)
    row = lax.broadcasted_iota(jnp.int32, (rows, tokens), 0)
    weights = affinity / jnp.sum(affinity, 0, keepdims=True)
    back = back_ref[...].reshape(rows, x_ref.shape[1])
    total = x_ref[...].astype(jnp.float32)
    for k in range(2):
        begin = routes[k : k + 1, :] * capacity
        mine = pick & (row >= begin) & (row < begin + capacity)
        picked = lax.dot_general(
            as_bf16(mine), back, (((0,), (0,)), ((), ())), preferred_element_type=jnp.float32
        )
        weight = jnp.broadcast_to(weights[k : k + 1, :], (tokens, tokens)).T[:, 0:1]
        total = total + weight * picked
    out_ref[...] = total.astype(jnp.bfloat16)


def layer(
    x_fwd,
    routes_fwd,
    affinity_fwd,
    x_bwd,
    grad_bwd,
    routes_bwd,
    affinity_bwd,
    up_weight,
    down_weight,
):
    devices = lax.axis_size("expert")
    experts = devices // 2
    tokens = x_fwd.shape[1]
    model_width = x_fwd.shape[2]
    top_count = routes_fwd.shape[2]
    capacity = 3 * tokens * top_count // devices
    rows = experts * capacity
    groups = same_side_groups(devices)
    params = pltpu.CompilerParams(vmem_limit_bytes=60 * 1024 * 1024)

    up_own = up_weight[0]
    down_own = down_weight[0]
    up_other = from_partner(up_own, "expert")
    down_other = from_partner(down_own, "expert")

    routes_f = routes_fwd[0].T
    routes_b = routes_bwd[0].T

    def exchange(block):
        return lax.all_to_all(
            block, "expert", split_axis=0, concat_axis=0, tiled=True, axis_index_groups=groups
        )

    send_f = pl.pallas_call(
        functools.partial(dispatch_fwd_kernel, capacity, experts),
        out_shape=jax.ShapeDtypeStruct((rows // 4, 4, model_width), jnp.bfloat16),
        in_specs=[VMEM] * 2,
        out_specs=VMEM,
        compiler_params=params,
        name="dispatch_fwd",
    )(routes_f, x_fwd[0])
    recv_f = exchange(send_f)
    send_b = pl.pallas_call(
        functools.partial(dispatch_bwd_kernel, capacity, experts),
        out_shape=jax.ShapeDtypeStruct((rows // 2, 4, model_width), jnp.bfloat16),
        in_specs=[VMEM] * 3,
        out_specs=VMEM,
        compiler_params=params,
        name="dispatch_bwd",
    )(routes_b, x_bwd[0], grad_bwd[0])
    recv_b = exchange(send_b)

    half = up_own.shape[1]

    def serve(kernel, received):
        return pl.pallas_call(
            kernel,
            out_shape=jax.ShapeDtypeStruct((rows // 4, 4, model_width), jnp.bfloat16),
            in_specs=[VMEM] + [ANY] * 4,
            out_specs=VMEM,
            scratch_shapes=[
                pltpu.VMEM((2, model_width, half), jnp.bfloat16),
                pltpu.VMEM((2, half, model_width), jnp.bfloat16),
                pltpu.VMEM((rows, 2 * half), jnp.bfloat16),
                pltpu.SemaphoreType.DMA((4,)),
            ],
            compiler_params=params,
        )(received, up_own, down_own, up_other, down_other)

    def combine(info, x, back):
        return pl.pallas_call(
            functools.partial(combine_kernel, capacity, experts),
            out_shape=jax.ShapeDtypeStruct((tokens, model_width), jnp.bfloat16),
            in_specs=[VMEM] * 3,
            out_specs=VMEM,
            compiler_params=params,
        )(info, x, back)

    def info_of(routes, affinity):
        return jnp.concatenate([routes.astype(jnp.float32), affinity[0].T], 0)

    x_f = shifted(x_fwd[0], "section", 1)
    x_b = shifted(grad_bwd[0], "section", -1)
    info_f = shifted(info_of(routes_f, affinity_fwd), "section", 1)
    info_b = shifted(info_of(routes_b, affinity_bwd), "section", -1)

    served_f = serve(expert_fwd_kernel, recv_f)
    served_f = shifted(served_f, "section", 1)
    back_f = exchange(served_f)
    served_b = serve(expert_bwd_kernel, recv_b)
    served_b = shifted(served_b, "section", -1)
    back_b = exchange(served_b)

    fwd_next = combine(info_f, x_f, back_f)
    bwd_next = combine(info_b, x_b, back_b)
    return (fwd_next[None], bwd_next[None])


def solution(mesh):
    rows = P("section", "expert", None)
    in_specs = (rows,) * 7 + (P("section", None, "expert"), rows)
    return jax.shard_map(
        layer, mesh=mesh, in_specs=in_specs, out_specs=(rows, rows), check_vma=False
    )
```

```python
import functools

import jax
import jax.numpy as jnp
from jax import lax
from jax.experimental import pallas as pl
from jax.experimental.pallas import tpu as pltpu
from jax.sharding import PartitionSpec as P


VMEM = pl.BlockSpec(memory_space=pltpu.VMEM)
ANY = pl.BlockSpec(memory_space=pl.ANY)
AGAINST_ROWS = (((1,), (1,)), ((), ()))
STEP = 512
WIDE = 512


def same_side_groups(devices):
    sides = [0 if d % 4 in (0, 3) else 1 for d in range(devices)]
    return [[d for d in range(devices) if sides[d] == side] for side in (0, 1)]


def from_partner(block, axis):
    count = lax.axis_size(axis)
    return lax.ppermute(block, axis, [(i, i ^ 1) for i in range(count)])


def shifted(shard, axis, by):
    size = lax.axis_size(axis)
    return lax.ppermute(shard, axis, [(i, (i + by) % size) for i in range(size)])


def silu_grad(values):
    sigma = jax.nn.sigmoid(values)
    return sigma * (1.0 + values * (1.0 - sigma))


def place_of(routes, experts):
    tokens = routes.shape[1]
    expert_id = lax.broadcasted_iota(jnp.int32, (experts, tokens), 0)
    named = (expert_id == routes[0:1, :]) | (expert_id == routes[1:2, :])
    earlier = (
        lax.broadcasted_iota(jnp.int32, (tokens, tokens), 0)
        < lax.broadcasted_iota(jnp.int32, (tokens, tokens), 1)
    )
    before = jnp.dot(
        named.astype(jnp.float32).astype(jnp.bfloat16),
        earlier.astype(jnp.float32).astype(jnp.bfloat16),
        preferred_element_type=jnp.float32,
    )
    return jnp.where(named, before, -1.0)


def slot_rows(place, block, first, capacity):
    experts, _ = place.shape
    rows = experts * block
    row = lax.broadcasted_iota(jnp.int32, (rows, experts), 0)
    col = lax.broadcasted_iota(jnp.int32, (rows, experts), 1)
    begin = col * block + first
    mine = (row >= begin) & (row < begin + capacity)
    spread = mine.astype(jnp.float32).astype(jnp.bfloat16)
    within = jnp.sum(jnp.where(mine, row - begin + 1, 0).astype(jnp.float32), 1, keepdims=True) - 1.0
    slot = jnp.dot(
        spread, (place + 1.0).astype(jnp.bfloat16), preferred_element_type=jnp.float32
    ) - 1.0
    return (slot == within) & (within >= 0.0)


def as_bf16(mask):
    return mask.astype(jnp.float32).astype(jnp.bfloat16)


def write_groups(out_ref, first, rows, members):
    experts, groups = members, rows.shape[0] // members // 4
    blocks = rows.reshape(experts, groups, 4, rows.shape[1])
    out_ref[:, first : first + groups] = blocks.astype(jnp.bfloat16)


def dispatch_kernel(capacity, experts, count, *refs):
    routes_ref, x_refs, out_ref, pick_ref = refs[0], refs[1 : 1 + count], refs[-2], refs[-1]

    @pl.when(pl.program_id(0) == 0)
    def _():
        place = place_of(routes_ref[...], experts)
        pick_ref[...] = as_bf16(slot_rows(place, capacity, 0, capacity))

    for i, x_ref in enumerate(x_refs):
        rows = jnp.dot(pick_ref[...], x_ref[...], preferred_element_type=jnp.float32)
        write_groups(out_ref, i * capacity // 4, rows, experts)


def start_loads(up_own, down_own, up_other, down_other, ups, downs, sems):
    pairs = ((up_own, ups.at[0]), (down_own, downs.at[0]), (up_other, ups.at[1]), (down_other, downs.at[1]))
    loads = [pltpu.make_async_copy(src, dst, sems.at[i]) for i, (src, dst) in enumerate(pairs)]
    for load in loads:
        load.start()
    return loads


def expert_fwd_kernel(
    recv_ref, up_own, down_own, up_other, down_other, out_ref, ups, downs, hidden, sems
):
    groups, per_group, width = out_ref.shape
    rows = groups * per_group
    half = hidden.shape[1] // 2
    loads = start_loads(up_own, down_own, up_other, down_other, ups, downs, sems)
    x = recv_ref[...].reshape(rows, width)
    for i in range(2):
        loads[2 * i].wait()
        pre_act = jnp.dot(x, ups[i], preferred_element_type=jnp.float32)
        hidden[:, i * half : (i + 1) * half] = jax.nn.silu(pre_act).astype(jnp.bfloat16)
    loads[1].wait()
    loads[3].wait()
    for c in range(0, width, STEP):
        part = jnp.dot(
            hidden[:, :half], downs[0, :, c : c + STEP], preferred_element_type=jnp.float32
        )
        part = part + jnp.dot(
            hidden[:, half:], downs[1, :, c : c + STEP], preferred_element_type=jnp.float32
        )
        out_ref[:, :, c : c + STEP] = part.reshape(groups, per_group, STEP).astype(jnp.bfloat16)


def expert_bwd_kernel(
    recv_ref, up_own, down_own, up_other, down_other, out_ref, ups, downs, hidden, sems
):
    groups, per_group, width = out_ref.shape
    rows = groups * per_group
    half = hidden.shape[1] // 2
    loads = start_loads(up_own, down_own, up_other, down_other, ups, downs, sems)
    sources = hidden.shape[1] // 32
    both = recv_ref[...].reshape(sources, 2 * groups // sources, per_group, width)
    x = both[:, : groups // sources].reshape(rows, width)
    g = both[:, groups // sources :].reshape(rows, width)
    for i in range(2):
        loads[2 * i].wait()
        pre_act = jnp.dot(x, ups[i], preferred_element_type=jnp.float32)
        loads[2 * i + 1].wait()
        hidden_grad = lax.dot_general(
            g, downs[i], AGAINST_ROWS, preferred_element_type=jnp.float32
        )
        pre_grad = hidden_grad * silu_grad(pre_act)
        hidden[:, i * half : (i + 1) * half] = pre_grad.astype(jnp.bfloat16)
    for c in range(0, width, STEP):
        part = lax.dot_general(
            hidden[:, :half], ups[0, c : c + STEP, :], AGAINST_ROWS,
            preferred_element_type=jnp.float32,
        )
        part = part + lax.dot_general(
            hidden[:, half:], ups[1, c : c + STEP, :], AGAINST_ROWS,
            preferred_element_type=jnp.float32,
        )
        out_ref[:, :, c : c + STEP] = part.reshape(groups, per_group, STEP).astype(jnp.bfloat16)


def combine_kernel(capacity, experts, info_ref, x_ref, back_ref, out_ref, pick_ref, weight_ref):
    tokens = x_ref.shape[0]
    rows = experts * capacity

    @pl.when(pl.program_id(0) == 0)
    def _():
        routes = info_ref[0:2, :].astype(jnp.int32)
        affinity = info_ref[2:4, :]
        pick = slot_rows(place_of(routes, experts), capacity, 0, capacity)
        row = lax.broadcasted_iota(jnp.int32, (rows, tokens), 0)
        weights = affinity / jnp.sum(affinity, 0, keepdims=True)
        for k in range(2):
            begin = routes[k : k + 1, :] * capacity
            mine = pick & (row >= begin) & (row < begin + capacity)
            pick_ref[k * tokens : (k + 1) * tokens, :] = as_bf16(mine).T
            weight_ref[k] = jnp.broadcast_to(weights[k : k + 1, :], (tokens, tokens)).T

    back = back_ref[...].reshape(rows, x_ref.shape[1])
    picked = jnp.dot(pick_ref[...], back, preferred_element_type=jnp.float32)
    total = x_ref[...].astype(jnp.float32)
    for k in range(2):
        total = total + weight_ref[k, :, 0:1] * picked[k * tokens : (k + 1) * tokens]
    out_ref[...] = total.astype(jnp.bfloat16)


def layer(
    x_fwd,
    routes_fwd,
    affinity_fwd,
    x_bwd,
    grad_bwd,
    routes_bwd,
    affinity_bwd,
    up_weight,
    down_weight,
):
    devices = lax.axis_size("expert")
    experts = devices // 2
    tokens = x_fwd.shape[1]
    model_width = x_fwd.shape[2]
    top_count = routes_fwd.shape[2]
    capacity = 3 * tokens * top_count // devices
    rows = experts * capacity
    groups = same_side_groups(devices)
    params = pltpu.CompilerParams(vmem_limit_bytes=60 * 1024 * 1024)

    up_own = up_weight[0]
    down_own = down_weight[0]
    up_other = from_partner(up_own, "expert")
    down_other = from_partner(down_own, "expert")

    routes_f = routes_fwd[0].T
    routes_b = routes_bwd[0].T

    def exchange(block):
        return lax.all_to_all(
            block, "expert", split_axis=0, concat_axis=0, tiled=True, axis_index_groups=groups
        )

    def dispatch(routes, blocks):
        count = len(blocks)
        groups_out = count * capacity // 4
        sent = pl.pallas_call(
            functools.partial(dispatch_kernel, capacity, experts, count),
            grid=(model_width // WIDE,),
            out_shape=jax.ShapeDtypeStruct((experts, groups_out, 4, model_width), jnp.bfloat16),
            in_specs=[pl.BlockSpec((top_count, tokens), lambda i: (0, 0))]
            + [pl.BlockSpec((tokens, WIDE), lambda i: (0, i))] * count,
            out_specs=pl.BlockSpec((experts, groups_out, 4, WIDE), lambda i: (0, 0, 0, i)),
            scratch_shapes=[pltpu.VMEM((rows, tokens), jnp.bfloat16)],
            compiler_params=params,
        )(routes, *blocks)
        return sent.reshape(experts * groups_out, 4, model_width)

    recv_b = exchange(dispatch(routes_b, (x_bwd[0], grad_bwd[0])))
    recv_f = exchange(dispatch(routes_f, (x_fwd[0],)))

    half = up_own.shape[1]

    def serve(kernel, received):
        return pl.pallas_call(
            kernel,
            out_shape=jax.ShapeDtypeStruct((rows // 4, 4, model_width), jnp.bfloat16),
            in_specs=[VMEM] + [ANY] * 4,
            out_specs=VMEM,
            scratch_shapes=[
                pltpu.VMEM((2, model_width, half), jnp.bfloat16),
                pltpu.VMEM((2, half, model_width), jnp.bfloat16),
                pltpu.VMEM((rows, 2 * half), jnp.bfloat16),
                pltpu.SemaphoreType.DMA((4,)),
            ],
            compiler_params=params,
        )(received, up_own, down_own, up_other, down_other)

    def combine(info, x, back):
        return pl.pallas_call(
            functools.partial(combine_kernel, capacity, experts),
            grid=(model_width // WIDE,),
            out_shape=jax.ShapeDtypeStruct((tokens, model_width), jnp.bfloat16),
            in_specs=[
                pl.BlockSpec((2 * top_count, tokens), lambda i: (0, 0)),
                pl.BlockSpec((tokens, WIDE), lambda i: (0, i)),
                pl.BlockSpec((rows // 4, 4, WIDE), lambda i: (0, 0, i)),
            ],
            out_specs=pl.BlockSpec((tokens, WIDE), lambda i: (0, i)),
            scratch_shapes=[
                pltpu.VMEM((top_count * tokens, rows), jnp.bfloat16),
                pltpu.VMEM((top_count, tokens, tokens), jnp.float32),
            ],
            compiler_params=params,
        )(info, x, back)

    def info_of(routes, affinity):
        return jnp.concatenate([routes.astype(jnp.float32), affinity[0].T], 0)

    served_b = serve(expert_bwd_kernel, recv_b)
    back_b = exchange(served_b)

    x_next = shifted(x_fwd[0], "section", 1)
    info_next = shifted(info_of(routes_f, affinity_fwd), "section", 1)
    served_f = serve(expert_fwd_kernel, recv_f)
    served_f = shifted(served_f, "section", 1)
    back_f = exchange(served_f)

    input_grad = combine(info_of(routes_b, affinity_bwd), grad_bwd[0], back_b)
    bwd_next = shifted(input_grad[None], "section", -1)
    fwd_next = combine(info_next, x_next, back_f)
    return (fwd_next[None], bwd_next)


def solution(mesh):
    rows = P("section", "expert", None)
    in_specs = (rows,) * 7 + (P("section", None, "expert"), rows)
    return jax.shard_map(
        layer, mesh=mesh, in_specs=in_specs, out_specs=(rows, rows), check_vma=False
    )
```

```python
import functools

import jax
import jax.numpy as jnp
from jax import lax
from jax.experimental import pallas as pl
from jax.experimental.pallas import tpu as pltpu
from jax.sharding import PartitionSpec as P


VMEM = pl.BlockSpec(memory_space=pltpu.VMEM)
ANY = pl.BlockSpec(memory_space=pl.ANY)
AGAINST_ROWS = (((1,), (1,)), ((), ()))
STEP = 512
WIDE = 1792


def same_side_groups(devices):
    sides = [0 if d % 4 in (0, 3) else 1 for d in range(devices)]
    return [[d for d in range(devices) if sides[d] == side] for side in (0, 1)]


def from_partner(block, axis):
    count = lax.axis_size(axis)
    return lax.ppermute(block, axis, [(i, i ^ 1) for i in range(count)])


def shifted(shard, axis, by):
    size = lax.axis_size(axis)
    return lax.ppermute(shard, axis, [(i, (i + by) % size) for i in range(size)])


def silu_grad(values):
    sigma = jax.nn.sigmoid(values)
    return sigma * (1.0 + values * (1.0 - sigma))


def place_of(routes, experts):
    tokens = routes.shape[1]
    expert_id = lax.broadcasted_iota(jnp.int32, (experts, tokens), 0)
    named = (expert_id == routes[0:1, :]) | (expert_id == routes[1:2, :])
    earlier = (
        lax.broadcasted_iota(jnp.int32, (tokens, tokens), 0)
        < lax.broadcasted_iota(jnp.int32, (tokens, tokens), 1)
    )
    before = jnp.dot(
        named.astype(jnp.float32).astype(jnp.bfloat16),
        earlier.astype(jnp.float32).astype(jnp.bfloat16),
        preferred_element_type=jnp.float32,
    )
    return jnp.where(named, before, -1.0)


def slot_rows(place, capacity):
    experts, tokens = place.shape
    rows = experts * capacity
    row = lax.broadcasted_iota(jnp.int32, (rows, experts), 0)
    begin = lax.broadcasted_iota(jnp.int32, (rows, experts), 1) * capacity
    spread = as_bf16((row >= begin) & (row < begin + capacity))
    slot = jnp.dot(spread, place.astype(jnp.bfloat16), preferred_element_type=jnp.float32)
    row = lax.broadcasted_iota(jnp.int32, (rows, tokens), 0)
    return slot == lax.rem(row, capacity).astype(jnp.float32)


def as_bf16(mask):
    return mask.astype(jnp.float32).astype(jnp.bfloat16)


def write_groups(out_ref, first, rows, members):
    experts, groups = members, rows.shape[0] // members // 4
    blocks = rows.reshape(experts, groups, 4, rows.shape[1])
    out_ref[:, first : first + groups] = blocks.astype(jnp.bfloat16)


def dispatch_kernel(capacity, experts, count, *refs):
    routes_ref, x_refs, out_ref, pick_ref = refs[0], refs[1 : 1 + count], refs[-2], refs[-1]

    @pl.when(pl.program_id(0) == 0)
    def _():
        place = place_of(routes_ref[...], experts)
        pick_ref[...] = as_bf16(slot_rows(place, capacity))

    for i, x_ref in enumerate(x_refs):
        rows = jnp.dot(pick_ref[...], x_ref[...], preferred_element_type=jnp.float32)
        write_groups(out_ref, i * capacity // 4, rows, experts)


def start_loads(up_own, down_own, up_other, down_other, ups, downs, sems):
    pairs = ((up_own, ups.at[0]), (down_own, downs.at[0]), (up_other, ups.at[1]), (down_other, downs.at[1]))
    loads = [pltpu.make_async_copy(src, dst, sems.at[i]) for i, (src, dst) in enumerate(pairs)]
    for load in loads:
        load.start()
    return loads


def expert_fwd_kernel(
    recv_ref, up_own, down_own, up_other, down_other, out_ref, ups, downs, hidden, sems
):
    groups, per_group, width = out_ref.shape
    rows = groups * per_group
    half = hidden.shape[1] // 2
    loads = start_loads(up_own, down_own, up_other, down_other, ups, downs, sems)
    x = recv_ref[...].reshape(rows, width)
    for i in range(2):
        loads[2 * i].wait()
        pre_act = jnp.dot(x, ups[i], preferred_element_type=jnp.float32)
        hidden[:, i * half : (i + 1) * half] = jax.nn.silu(pre_act).astype(jnp.bfloat16)
    loads[1].wait()
    loads[3].wait()
    for c in range(0, width, STEP):
        part = jnp.dot(
            hidden[:, :half], downs[0, :, c : c + STEP], preferred_element_type=jnp.float32
        )
        part = part + jnp.dot(
            hidden[:, half:], downs[1, :, c : c + STEP], preferred_element_type=jnp.float32
        )
        out_ref[:, :, c : c + STEP] = part.reshape(groups, per_group, STEP).astype(jnp.bfloat16)


def expert_bwd_kernel(
    recv_ref, up_own, down_own, up_other, down_other, out_ref, ups, downs, hidden, sems
):
    groups, per_group, width = out_ref.shape
    rows = groups * per_group
    half = hidden.shape[1] // 2
    loads = start_loads(up_own, down_own, up_other, down_other, ups, downs, sems)
    sources = hidden.shape[1] // 32
    both = recv_ref[...].reshape(sources, 2 * groups // sources, per_group, width)
    x = both[:, : groups // sources].reshape(rows, width)
    g = both[:, groups // sources :].reshape(rows, width)
    for i in range(2):
        loads[2 * i].wait()
        pre_act = jnp.dot(x, ups[i], preferred_element_type=jnp.float32)
        loads[2 * i + 1].wait()
        hidden_grad = lax.dot_general(
            g, downs[i], AGAINST_ROWS, preferred_element_type=jnp.float32
        )
        pre_grad = hidden_grad * silu_grad(pre_act)
        hidden[:, i * half : (i + 1) * half] = pre_grad.astype(jnp.bfloat16)
    for c in range(0, width, STEP):
        part = lax.dot_general(
            hidden[:, :half], ups[0, c : c + STEP, :], AGAINST_ROWS,
            preferred_element_type=jnp.float32,
        )
        part = part + lax.dot_general(
            hidden[:, half:], ups[1, c : c + STEP, :], AGAINST_ROWS,
            preferred_element_type=jnp.float32,
        )
        out_ref[:, :, c : c + STEP] = part.reshape(groups, per_group, STEP).astype(jnp.bfloat16)


def recipe_kernel(capacity, experts, info_ref, pick_ref, weight_ref):
    routes = info_ref[0:2, :].astype(jnp.int32)
    affinity = info_ref[2:4, :]
    tokens = routes.shape[1]
    rows = experts * capacity
    pick = slot_rows(place_of(routes, experts), capacity)
    row = lax.broadcasted_iota(jnp.int32, (rows, tokens), 0)
    weights = affinity / jnp.sum(affinity, 0, keepdims=True)
    for k in range(2):
        begin = routes[k : k + 1, :] * capacity
        mine = pick & (row >= begin) & (row < begin + capacity)
        pick_ref[k * tokens : (k + 1) * tokens, :] = as_bf16(mine).T
        weight_ref[k] = jnp.broadcast_to(weights[k : k + 1, :], (tokens, tokens)).T


def combine_kernel(pick_ref, weight_ref, x_ref, back_ref, out_ref):
    tokens = x_ref.shape[0]
    back = back_ref[...].reshape(pick_ref.shape[1], x_ref.shape[1])
    picked = jnp.dot(pick_ref[...], back, preferred_element_type=jnp.float32)
    total = x_ref[...].astype(jnp.float32)
    for k in range(2):
        total = total + weight_ref[k, :, 0:1] * picked[k * tokens : (k + 1) * tokens]
    out_ref[...] = total.astype(jnp.bfloat16)


def settle_kernel(in_ref, out_ref):
    out_ref[...] = in_ref[...]


def layer(
    x_fwd,
    routes_fwd,
    affinity_fwd,
    x_bwd,
    grad_bwd,
    routes_bwd,
    affinity_bwd,
    up_weight,
    down_weight,
):
    devices = lax.axis_size("expert")
    experts = devices // 2
    tokens = x_fwd.shape[1]
    model_width = x_fwd.shape[2]
    top_count = routes_fwd.shape[2]
    capacity = 3 * tokens * top_count // devices
    rows = experts * capacity
    groups = same_side_groups(devices)
    params = pltpu.CompilerParams(vmem_limit_bytes=63 * 1024 * 1024)

    up_own = up_weight[0]
    down_own = down_weight[0]
    up_other = from_partner(up_own, "expert")
    down_other = from_partner(down_own, "expert")

    routes_f = routes_fwd[0].T
    routes_b = routes_bwd[0].T

    def exchange(block):
        return lax.all_to_all(
            block, "expert", split_axis=0, concat_axis=0, tiled=True, axis_index_groups=groups
        )

    def dispatch(routes, blocks):
        count = len(blocks)
        groups_out = count * capacity // 4
        sent = pl.pallas_call(
            functools.partial(dispatch_kernel, capacity, experts, count),
            grid=(model_width // WIDE,),
            out_shape=jax.ShapeDtypeStruct((experts, groups_out, 4, model_width), jnp.bfloat16),
            in_specs=[pl.BlockSpec((top_count, tokens), lambda i: (0, 0))]
            + [pl.BlockSpec((tokens, WIDE), lambda i: (0, i))] * count,
            out_specs=pl.BlockSpec((experts, groups_out, 4, WIDE), lambda i: (0, 0, 0, i)),
            scratch_shapes=[pltpu.VMEM((rows, tokens), jnp.bfloat16)],
            compiler_params=params,
        )(routes, *blocks)
        return sent.reshape(experts * groups_out, 4, model_width)

    recv_b = exchange(dispatch(routes_b, (x_bwd[0], grad_bwd[0])))
    recv_f = exchange(dispatch(routes_f, (x_fwd[0],)))

    half = up_own.shape[1]

    def serve(kernel, received):
        return pl.pallas_call(
            kernel,
            out_shape=jax.ShapeDtypeStruct((rows // 4, 4, model_width), jnp.bfloat16),
            in_specs=[VMEM] + [ANY] * 4,
            out_specs=VMEM,
            scratch_shapes=[
                pltpu.VMEM((2, model_width, half), jnp.bfloat16),
                pltpu.VMEM((2, half, model_width), jnp.bfloat16),
                pltpu.VMEM((rows, 2 * half), jnp.bfloat16),
                pltpu.SemaphoreType.DMA((4,)),
            ],
            compiler_params=params,
        )(received, up_own, down_own, up_other, down_other)

    def recipe(info):
        return pl.pallas_call(
            functools.partial(recipe_kernel, capacity, experts),
            out_shape=(
                jax.ShapeDtypeStruct((top_count * tokens, rows), jnp.bfloat16),
                jax.ShapeDtypeStruct((top_count, tokens, tokens), jnp.float32),
            ),
            in_specs=[VMEM],
            out_specs=(VMEM, VMEM),
            compiler_params=params,
        )(info)

    def combine(pick_and_weight, x, back):
        return pl.pallas_call(
            combine_kernel,
            grid=(model_width // WIDE,),
            out_shape=jax.ShapeDtypeStruct((tokens, model_width), jnp.bfloat16),
            in_specs=[
                pl.BlockSpec((top_count * tokens, rows), lambda i: (0, 0)),
                pl.BlockSpec((top_count, tokens, tokens), lambda i: (0, 0, 0)),
                pl.BlockSpec((tokens, WIDE), lambda i: (0, i)),
                pl.BlockSpec((rows // 4, 4, WIDE), lambda i: (0, 0, i)),
            ],
            out_specs=pl.BlockSpec((tokens, WIDE), lambda i: (0, i)),
            compiler_params=params,
        )(*pick_and_weight, x, back)

    def settle(block):
        return pl.pallas_call(
            settle_kernel,
            out_shape=jax.ShapeDtypeStruct(block.shape, block.dtype),
            in_specs=[VMEM],
            out_specs=VMEM,
        )(block)

    def info_of(routes, affinity):
        return jnp.concatenate([routes.astype(jnp.float32), affinity[0].T], 0)

    served_b = serve(expert_bwd_kernel, recv_b)
    back_b = exchange(served_b)

    x_next = shifted(x_fwd[0], "section", 1)
    info_next = shifted(info_of(routes_f, affinity_fwd), "section", 1)
    served_f = serve(expert_fwd_kernel, recv_f)
    served_f = shifted(served_f, "section", 1)
    back_f = exchange(served_f)

    recipe_b = recipe(info_of(routes_b, affinity_bwd))
    recipe_f = recipe(info_next)
    input_grad = combine(recipe_b, grad_bwd[0], back_b)
    bwd_next = shifted(input_grad, "section", -1)
    bwd_next = settle(bwd_next)
    fwd_next = combine(recipe_f, x_next, back_f)
    return (fwd_next[None], bwd_next[None])


def solution(mesh):
    rows = P("section", "expert", None)
    in_specs = (rows,) * 7 + (P("section", None, "expert"), rows)
    return jax.shard_map(
        layer, mesh=mesh, in_specs=in_specs, out_specs=(rows, rows), check_vma=False
    )
```

```python
import functools

import jax
import jax.numpy as jnp
from jax import lax
from jax.experimental import pallas as pl
from jax.experimental.pallas import tpu as pltpu
from jax.sharding import PartitionSpec as P


VMEM = pl.BlockSpec(memory_space=pltpu.VMEM)
ANY = pl.BlockSpec(memory_space=pl.ANY)
AGAINST_ROWS = (((1,), (1,)), ((), ()))
STEP = 512
BATCHES = ((4, 3, 5, 0), (2, 6, 1, 7))
WIDE = 1792


def same_side_groups(devices):
    sides = [0 if d % 4 in (0, 3) else 1 for d in range(devices)]
    return [[d for d in range(devices) if sides[d] == side] for side in (0, 1)]


def from_partner(block, axis):
    count = lax.axis_size(axis)
    return lax.ppermute(block, axis, [(i, i ^ 1) for i in range(count)])


def shifted(shard, axis, by):
    size = lax.axis_size(axis)
    return lax.ppermute(shard, axis, [(i, (i + by) % size) for i in range(size)])


def silu_grad(values):
    sigma = jax.nn.sigmoid(values)
    return sigma * (1.0 + values * (1.0 - sigma))


def place_of(routes, experts):
    tokens = routes.shape[1]
    expert_id = lax.broadcasted_iota(jnp.int32, (experts, tokens), 0)
    named = (expert_id == routes[0:1, :]) | (expert_id == routes[1:2, :])
    earlier = (
        lax.broadcasted_iota(jnp.int32, (tokens, tokens), 0)
        < lax.broadcasted_iota(jnp.int32, (tokens, tokens), 1)
    )
    before = jnp.dot(
        named.astype(jnp.float32).astype(jnp.bfloat16),
        earlier.astype(jnp.float32).astype(jnp.bfloat16),
        preferred_element_type=jnp.float32,
    )
    return jnp.where(named, before, -1.0)


def slot_rows(place, capacity):
    experts, tokens = place.shape
    rows = experts * capacity
    row = lax.broadcasted_iota(jnp.int32, (rows, experts), 0)
    begin = lax.broadcasted_iota(jnp.int32, (rows, experts), 1) * capacity
    spread = as_bf16((row >= begin) & (row < begin + capacity))
    slot = jnp.dot(spread, place.astype(jnp.bfloat16), preferred_element_type=jnp.float32)
    row = lax.broadcasted_iota(jnp.int32, (rows, tokens), 0)
    return slot == lax.rem(row, capacity).astype(jnp.float32)


def as_bf16(mask):
    return mask.astype(jnp.float32).astype(jnp.bfloat16)


def write_groups(out_ref, first, rows, members):
    experts, groups = members, rows.shape[0] // members // 4
    blocks = rows.reshape(experts, groups, 4, rows.shape[1])
    out_ref[:, first : first + groups] = blocks.astype(jnp.bfloat16)


def dispatch_kernel(capacity, experts, count, *refs):
    routes_ref, x_refs, out_ref, pick_ref = refs[0], refs[1 : 1 + count], refs[-2], refs[-1]

    @pl.when(pl.program_id(0) == 0)
    def _():
        place = place_of(routes_ref[...], experts)
        pick_ref[...] = as_bf16(slot_rows(place, capacity))

    for i, x_ref in enumerate(x_refs):
        rows = jnp.dot(pick_ref[...], x_ref[...], preferred_element_type=jnp.float32)
        write_groups(out_ref, i * capacity // 4, rows, experts)


def relative_routes(routes):
    me = lax.axis_index("expert")
    x, z, member = me // 32, (me // 4) % 8, (me % 4) // 2
    plane = ((routes // 2) % 8 - z + 8) % 8
    return plane * 4 + ((routes // 16) ^ x) * 2 + ((routes % 2) ^ member)


def dispatch_planes_kernel(capacity, experts, routes_ref, x_ref, g_ref, *refs):
    out_refs, pick_ref = refs[:-1], refs[-1]

    @pl.when(pl.program_id(0) == 0)
    def _():
        place = place_of(relative_routes(routes_ref[...]), experts)
        pick_ref[...] = as_bf16(slot_rows(place, capacity))

    planes = len(out_refs)
    members, groups = experts // planes, capacity // 4
    for i, rows_ref in enumerate((x_ref, g_ref)):
        rows = jnp.dot(pick_ref[...], rows_ref[...], preferred_element_type=jnp.float32)
        blocks = rows.reshape(planes, members, groups, 4, rows.shape[1]).astype(jnp.bfloat16)
        for k, out_ref in enumerate(out_refs):
            out_ref[:, i * groups : (i + 1) * groups] = blocks[k]


def regroup_kernel(block, *refs):
    count = (len(refs) - 1) // 2
    in_refs, out_refs, sems = refs[:count], refs[count : 2 * count], refs[-1]
    copies = []
    for i, out_ref in enumerate(out_refs):
        for k, in_ref in enumerate(in_refs):
            copies.append(
                pltpu.make_async_copy(
                    in_ref.at[pl.ds(i * block, block)],
                    out_ref.at[pl.ds(k * block, block)],
                    sems.at[i, k],
                )
            )
    for copy in copies:
        copy.start()
    for copy in copies:
        copy.wait()


def start_loads(up_own, down_own, up_other, down_other, ups, downs, sems):
    pairs = ((up_own, ups.at[0]), (down_own, downs.at[0]), (up_other, ups.at[1]), (down_other, downs.at[1]))
    loads = [pltpu.make_async_copy(src, dst, sems.at[i]) for i, (src, dst) in enumerate(pairs)]
    for load in loads:
        load.start()
    return loads


def expert_fwd_kernel(
    recv_ref, up_own, down_own, up_other, down_other, out_ref, ups, downs, hidden, sems
):
    groups, per_group, width = out_ref.shape
    rows = groups * per_group
    half = hidden.shape[1] // 2
    loads = start_loads(up_own, down_own, up_other, down_other, ups, downs, sems)
    x = recv_ref[...].reshape(rows, width)
    for i in range(2):
        loads[2 * i].wait()
        pre_act = jnp.dot(x, ups[i], preferred_element_type=jnp.float32)
        hidden[:, i * half : (i + 1) * half] = jax.nn.silu(pre_act).astype(jnp.bfloat16)
    loads[1].wait()
    loads[3].wait()
    for c in range(0, width, STEP):
        part = jnp.dot(
            hidden[:, :half], downs[0, :, c : c + STEP], preferred_element_type=jnp.float32
        )
        part = part + jnp.dot(
            hidden[:, half:], downs[1, :, c : c + STEP], preferred_element_type=jnp.float32
        )
        out_ref[:, :, c : c + STEP] = part.reshape(groups, per_group, STEP).astype(jnp.bfloat16)


def expert_bwd_kernel(batches, *refs):
    count = len(batches) * 4
    recv_refs = refs[:count]
    up_own, down_own, up_other, down_other, out_ref = refs[count : count + 5]
    ups, downs, hidden, sems, x_ref, g_ref = refs[count + 5 :]
    groups, per_group, width = out_ref.shape
    half = hidden.shape[1] // 2
    loads = start_loads(up_own, down_own, up_other, down_other, ups, downs, sems)
    planes = len(batches[0])
    each = x_ref.shape[0] // count
    for n, recv_ref in enumerate(recv_refs):
        both = recv_ref[...].reshape(planes, 2, each // planes // 4, per_group, width)
        x_ref[n * each : (n + 1) * each, :] = both[:, 0].reshape(each, width)
        g_ref[n * each : (n + 1) * each, :] = both[:, 1].reshape(each, width)
    for i in range(2):
        loads[2 * i].wait()
        pre_act = jnp.dot(x_ref[...], ups[i], preferred_element_type=jnp.float32)
        loads[2 * i + 1].wait()
        hidden_grad = lax.dot_general(
            g_ref[...], downs[i], AGAINST_ROWS, preferred_element_type=jnp.float32
        )
        pre_grad = hidden_grad * silu_grad(pre_act)
        hidden[:, i * half : (i + 1) * half] = pre_grad.astype(jnp.bfloat16)
    me = lax.axis_index("expert")
    x, z, member = me // 32, (me // 4) % 8, (me % 4) // 2
    sources = [
        (x ^ (i // 2)) * 16 + ((z - k + 8) % 8) * 2 + (member ^ (i % 2))
        for batch in batches
        for i in range(4)
        for k in batch
    ]
    piece = groups // len(sources)
    for c in range(0, width, STEP):
        part = lax.dot_general(
            hidden[:, :half], ups[0, c : c + STEP, :], AGAINST_ROWS,
            preferred_element_type=jnp.float32,
        )
        part = part + lax.dot_general(
            hidden[:, half:], ups[1, c : c + STEP, :], AGAINST_ROWS,
            preferred_element_type=jnp.float32,
        )
        blocks = part.reshape(len(sources), piece, per_group, STEP).astype(jnp.bfloat16)
        for n, source in enumerate(sources):
            out_ref[pl.ds(source * piece, piece), :, c : c + STEP] = blocks[n]


def recipe_kernel(capacity, experts, info_ref, pick_ref, weight_ref):
    routes = info_ref[0:2, :].astype(jnp.int32)
    affinity = info_ref[2:4, :]
    tokens = routes.shape[1]
    rows = experts * capacity
    pick = slot_rows(place_of(routes, experts), capacity)
    row = lax.broadcasted_iota(jnp.int32, (rows, tokens), 0)
    weights = affinity / jnp.sum(affinity, 0, keepdims=True)
    for k in range(2):
        begin = routes[k : k + 1, :] * capacity
        mine = pick & (row >= begin) & (row < begin + capacity)
        pick_ref[k * tokens : (k + 1) * tokens, :] = as_bf16(mine).T
        weight_ref[k] = jnp.broadcast_to(weights[k : k + 1, :], (tokens, tokens)).T


def combine_kernel(pick_ref, weight_ref, x_ref, back_ref, out_ref):
    tokens = x_ref.shape[0]
    back = back_ref[...].reshape(pick_ref.shape[1], x_ref.shape[1])
    picked = jnp.dot(pick_ref[...], back, preferred_element_type=jnp.float32)
    total = x_ref[...].astype(jnp.float32)
    for k in range(2):
        total = total + weight_ref[k, :, 0:1] * picked[k * tokens : (k + 1) * tokens]
    out_ref[...] = total.astype(jnp.bfloat16)


def settle_kernel(in_ref, out_ref):
    out_ref[...] = in_ref[...]


def layer(
    x_fwd,
    routes_fwd,
    affinity_fwd,
    x_bwd,
    grad_bwd,
    routes_bwd,
    affinity_bwd,
    up_weight,
    down_weight,
):
    devices = lax.axis_size("expert")
    experts = devices // 2
    tokens = x_fwd.shape[1]
    model_width = x_fwd.shape[2]
    top_count = routes_fwd.shape[2]
    capacity = 3 * tokens * top_count // devices
    rows = experts * capacity
    groups = same_side_groups(devices)
    params = pltpu.CompilerParams(vmem_limit_bytes=63 * 1024 * 1024)

    up_own = up_weight[0]
    down_own = down_weight[0]
    up_other = from_partner(up_own, "expert")
    down_other = from_partner(down_own, "expert")

    routes_f = routes_fwd[0].T
    routes_b = routes_bwd[0].T

    def exchange(block):
        return lax.all_to_all(
            block, "expert", split_axis=0, concat_axis=0, tiled=True, axis_index_groups=groups
        )

    def dispatch(routes, blocks):
        count = len(blocks)
        groups_out = count * capacity // 4
        sent = pl.pallas_call(
            functools.partial(dispatch_kernel, capacity, experts, count),
            grid=(model_width // WIDE,),
            out_shape=jax.ShapeDtypeStruct((experts, groups_out, 4, model_width), jnp.bfloat16),
            in_specs=[pl.BlockSpec((top_count, tokens), lambda i: (0, 0))]
            + [pl.BlockSpec((tokens, WIDE), lambda i: (0, i))] * count,
            out_specs=pl.BlockSpec((experts, groups_out, 4, WIDE), lambda i: (0, 0, 0, i)),
            scratch_shapes=[pltpu.VMEM((rows, tokens), jnp.bfloat16)],
            compiler_params=params,
        )(routes, *blocks)
        return sent.reshape(experts * groups_out, 4, model_width)

    groups_b = 2 * capacity // 4
    sent_b = pl.pallas_call(
        functools.partial(dispatch_planes_kernel, capacity, experts),
        grid=(model_width // WIDE,),
        out_shape=[jax.ShapeDtypeStruct((4, groups_b, 4, model_width), jnp.bfloat16)] * 8,
        in_specs=[pl.BlockSpec((top_count, tokens), lambda i: (0, 0))]
        + [pl.BlockSpec((tokens, WIDE), lambda i: (0, i))] * 2,
        out_specs=[pl.BlockSpec((4, groups_b, 4, WIDE), lambda i: (0, 0, 0, i))] * 8,
        scratch_shapes=[pltpu.VMEM((rows, tokens), jnp.bfloat16)],
        compiler_params=params,
        name="dispatch_bwd",
    )(routes_b, x_bwd[0], grad_bwd[0])
    sent_b = [block.reshape(4 * groups_b, 4, model_width) for block in sent_b]

    def along_z(block, k):
        pairs = [(d, d // 32 * 32 + (d + 4 * k) % 32) for d in range(devices)]
        return lax.ppermute(block, "expert", pairs)

    def in_plane(block, i):
        pairs = [
            (d, (d ^ (32 * (i // 2))) // 4 * 4 + (3 - d % 4 if i % 2 else d % 4))
            for d in range(devices)
        ]
        return lax.ppermute(block, "expert", pairs)

    def regroup(blocks):
        count = len(blocks)
        return pl.pallas_call(
            functools.partial(regroup_kernel, groups_b),
            out_shape=[jax.ShapeDtypeStruct(blocks[0].shape, jnp.bfloat16)] * count,
            in_specs=[ANY] * count,
            out_specs=[ANY] * count,
            scratch_shapes=[pltpu.SemaphoreType.DMA((count, count))],
            compiler_params=params,
        )(*blocks)

    arrived = {k: along_z(sent_b[k], k) for batch in BATCHES for k in batch if k}
    arrived[0] = sent_b[0]
    recv_b = []
    for batch in BATCHES:
        by_member = regroup([arrived[k] for k in batch])
        recv_b += [in_plane(block, i) if i else block for i, block in enumerate(by_member)]
    recv_f = exchange(dispatch(routes_f, (x_fwd[0],)))

    half = up_own.shape[1]

    def serve(kernel, received, extra=()):
        return pl.pallas_call(
            kernel,
            out_shape=jax.ShapeDtypeStruct((rows // 4, 4, model_width), jnp.bfloat16),
            in_specs=[VMEM] * len(received) + [ANY] * 4,
            out_specs=VMEM,
            scratch_shapes=[
                pltpu.VMEM((2, model_width, half), jnp.bfloat16),
                pltpu.VMEM((2, half, model_width), jnp.bfloat16),
                pltpu.VMEM((rows, 2 * half), jnp.bfloat16),
                pltpu.SemaphoreType.DMA((4,)),
                *extra,
            ],
            compiler_params=params,
        )(*received, up_own, down_own, up_other, down_other)

    def recipe(info):
        return pl.pallas_call(
            functools.partial(recipe_kernel, capacity, experts),
            out_shape=(
                jax.ShapeDtypeStruct((top_count * tokens, rows), jnp.bfloat16),
                jax.ShapeDtypeStruct((top_count, tokens, tokens), jnp.float32),
            ),
            in_specs=[VMEM],
            out_specs=(VMEM, VMEM),
            compiler_params=params,
        )(info)

    def combine(pick_and_weight, x, back):
        return pl.pallas_call(
            combine_kernel,
            grid=(model_width // WIDE,),
            out_shape=jax.ShapeDtypeStruct((tokens, model_width), jnp.bfloat16),
            in_specs=[
                pl.BlockSpec((top_count * tokens, rows), lambda i: (0, 0)),
                pl.BlockSpec((top_count, tokens, tokens), lambda i: (0, 0, 0)),
                pl.BlockSpec((tokens, WIDE), lambda i: (0, i)),
                pl.BlockSpec((rows // 4, 4, WIDE), lambda i: (0, 0, i)),
            ],
            out_specs=pl.BlockSpec((tokens, WIDE), lambda i: (0, i)),
            compiler_params=params,
        )(*pick_and_weight, x, back)

    def settle(block):
        return pl.pallas_call(
            settle_kernel,
            out_shape=jax.ShapeDtypeStruct(block.shape, block.dtype),
            in_specs=[VMEM],
            out_specs=VMEM,
        )(block)

    def info_of(routes, affinity):
        return jnp.concatenate([routes.astype(jnp.float32), affinity[0].T], 0)

    served_b = serve(
        functools.partial(expert_bwd_kernel, BATCHES),
        recv_b,
        [pltpu.VMEM((rows, model_width), jnp.bfloat16)] * 2,
    )
    back_b = exchange(served_b)

    x_next = shifted(x_fwd[0], "section", 1)
    info_next = shifted(info_of(routes_f, affinity_fwd), "section", 1)
    served_f = serve(expert_fwd_kernel, [recv_f])
    served_f = shifted(served_f, "section", 1)
    back_f = exchange(served_f)

    recipe_b = recipe(info_of(routes_b, affinity_bwd))
    recipe_f = recipe(info_next)
    input_grad = combine(recipe_b, grad_bwd[0], back_b)
    bwd_next = shifted(input_grad, "section", -1)
    bwd_next = settle(bwd_next)
    fwd_next = combine(recipe_f, x_next, back_f)
    return (fwd_next[None], bwd_next[None])


def solution(mesh):
    rows = P("section", "expert", None)
    in_specs = (rows,) * 7 + (P("section", None, "expert"), rows)
    return jax.shard_map(
        layer, mesh=mesh, in_specs=in_specs, out_specs=(rows, rows), check_vma=False
    )
```

```python
import functools

import jax
import jax.numpy as jnp
from jax import lax
from jax.experimental import pallas as pl
from jax.experimental.pallas import tpu as pltpu
from jax.sharding import PartitionSpec as P


VMEM = pl.BlockSpec(memory_space=pltpu.VMEM)
ANY = pl.BlockSpec(memory_space=pl.ANY)
AGAINST_ROWS = (((1,), (1,)), ((), ()))
STEP = 512
BATCHES = ((4, 0), (3, 5), (2, 6), (1, 7))
WIDE = 1792


def same_side_groups(devices):
    sides = [0 if d % 4 in (0, 3) else 1 for d in range(devices)]
    return [[d for d in range(devices) if sides[d] == side] for side in (0, 1)]


def from_partner(block, axis):
    count = lax.axis_size(axis)
    return lax.ppermute(block, axis, [(i, i ^ 1) for i in range(count)])


def shifted(shard, axis, by):
    size = lax.axis_size(axis)
    return lax.ppermute(shard, axis, [(i, (i + by) % size) for i in range(size)])


def silu_grad(values):
    sigma = jax.nn.sigmoid(values)
    return sigma * (1.0 + values * (1.0 - sigma))


def place_of(routes, experts):
    tokens = routes.shape[1]
    expert_id = lax.broadcasted_iota(jnp.int32, (experts, tokens), 0)
    named = (expert_id == routes[0:1, :]) | (expert_id == routes[1:2, :])
    earlier = (
        lax.broadcasted_iota(jnp.int32, (tokens, tokens), 0)
        < lax.broadcasted_iota(jnp.int32, (tokens, tokens), 1)
    )
    before = jnp.dot(
        named.astype(jnp.float32).astype(jnp.bfloat16),
        earlier.astype(jnp.float32).astype(jnp.bfloat16),
        preferred_element_type=jnp.float32,
    )
    return jnp.where(named, before, -1.0)


def slot_rows(place, capacity):
    experts, tokens = place.shape
    rows = experts * capacity
    row = lax.broadcasted_iota(jnp.int32, (rows, experts), 0)
    begin = lax.broadcasted_iota(jnp.int32, (rows, experts), 1) * capacity
    spread = as_bf16((row >= begin) & (row < begin + capacity))
    slot = jnp.dot(spread, place.astype(jnp.bfloat16), preferred_element_type=jnp.float32)
    row = lax.broadcasted_iota(jnp.int32, (rows, tokens), 0)
    return slot == lax.rem(row, capacity).astype(jnp.float32)


def as_bf16(mask):
    return mask.astype(jnp.float32).astype(jnp.bfloat16)


def write_groups(out_ref, first, rows, members):
    experts, groups = members, rows.shape[0] // members // 4
    blocks = rows.reshape(experts, groups, 4, rows.shape[1])
    out_ref[:, first : first + groups] = blocks.astype(jnp.bfloat16)


def dispatch_kernel(capacity, experts, count, *refs):
    routes_ref, x_refs, out_ref, pick_ref = refs[0], refs[1 : 1 + count], refs[-2], refs[-1]

    @pl.when(pl.program_id(0) == 0)
    def _():
        place = place_of(routes_ref[...], experts)
        pick_ref[...] = as_bf16(slot_rows(place, capacity))

    for i, x_ref in enumerate(x_refs):
        rows = jnp.dot(pick_ref[...], x_ref[...], preferred_element_type=jnp.float32)
        write_groups(out_ref, i * capacity // 4, rows, experts)


def relative_routes(routes):
    me = lax.axis_index("expert")
    x, z, member = me // 32, (me // 4) % 8, (me % 4) // 2
    plane = ((routes // 2) % 8 - z + 8) % 8
    return plane * 4 + ((routes // 16) ^ x) * 2 + ((routes % 2) ^ member)


def dispatch_planes_kernel(capacity, experts, routes_ref, x_ref, g_ref, *refs):
    out_refs, pick_ref = refs[:-1], refs[-1]

    @pl.when(pl.program_id(0) == 0)
    def _():
        place = place_of(relative_routes(routes_ref[...]), experts)
        pick_ref[...] = as_bf16(slot_rows(place, capacity))

    planes = len(out_refs)
    members, groups = experts // planes, capacity // 4
    for i, rows_ref in enumerate((x_ref, g_ref)):
        rows = jnp.dot(pick_ref[...], rows_ref[...], preferred_element_type=jnp.float32)
        blocks = rows.reshape(planes, members, groups, 4, rows.shape[1]).astype(jnp.bfloat16)
        for k, out_ref in enumerate(out_refs):
            out_ref[:, i * groups : (i + 1) * groups] = blocks[k]


def regroup_kernel(block, *refs):
    count = len(refs) - 7
    in_refs, out_refs = refs[:count], refs[count : count + 4]
    stage, in_sems, out_sems = refs[count + 4 :]
    loads, stores = [], []
    for i, out_ref in enumerate(out_refs):
        for k, in_ref in enumerate(in_refs):
            loads.append(
                pltpu.make_async_copy(
                    in_ref.at[pl.ds(i * block, block)],
                    stage.at[i, pl.ds(k * block, block)],
                    in_sems.at[i, k],
                )
            )
        stores.append(pltpu.make_async_copy(stage.at[i], out_ref, out_sems.at[i]))
    for load in loads:
        load.start()
    for i, store in enumerate(stores):
        for load in loads[i * count : (i + 1) * count]:
            load.wait()
        store.start()
    for store in stores:
        store.wait()


def start_loads(up_own, down_own, up_other, down_other, ups, downs, sems):
    pairs = ((up_own, ups.at[0]), (down_own, downs.at[0]), (up_other, ups.at[1]), (down_other, downs.at[1]))
    loads = [pltpu.make_async_copy(src, dst, sems.at[i]) for i, (src, dst) in enumerate(pairs)]
    for load in loads:
        load.start()
    return loads


def expert_fwd_kernel(
    recv_ref, up_own, down_own, up_other, down_other, out_ref, ups, downs, hidden, sems
):
    groups, per_group, width = out_ref.shape
    rows = groups * per_group
    half = hidden.shape[1] // 2
    loads = start_loads(up_own, down_own, up_other, down_other, ups, downs, sems)
    x = recv_ref[...].reshape(rows, width)
    for i in range(2):
        loads[2 * i].wait()
        pre_act = jnp.dot(x, ups[i], preferred_element_type=jnp.float32)
        hidden[:, i * half : (i + 1) * half] = jax.nn.silu(pre_act).astype(jnp.bfloat16)
    loads[1].wait()
    loads[3].wait()
    for c in range(0, width, STEP):
        part = jnp.dot(
            hidden[:, :half], downs[0, :, c : c + STEP], preferred_element_type=jnp.float32
        )
        part = part + jnp.dot(
            hidden[:, half:], downs[1, :, c : c + STEP], preferred_element_type=jnp.float32
        )
        out_ref[:, :, c : c + STEP] = part.reshape(groups, per_group, STEP).astype(jnp.bfloat16)


def expert_bwd_kernel(batches, *refs):
    count = len(batches) * 4
    recv_refs = refs[:count]
    up_own, down_own, up_other, down_other, out_ref = refs[count : count + 5]
    ups, downs, hidden, sems, x_ref, g_ref = refs[count + 5 :]
    groups, per_group, width = out_ref.shape
    half = hidden.shape[1] // 2
    loads = start_loads(up_own, down_own, up_other, down_other, ups, downs, sems)
    planes = len(batches[0])
    each = x_ref.shape[0] // count
    for n, recv_ref in enumerate(recv_refs):
        both = recv_ref[...].reshape(planes, 2, each // planes // 4, per_group, width)
        x_ref[n * each : (n + 1) * each, :] = both[:, 0].reshape(each, width)
        g_ref[n * each : (n + 1) * each, :] = both[:, 1].reshape(each, width)
    for i in range(2):
        loads[2 * i].wait()
        pre_act = jnp.dot(x_ref[...], ups[i], preferred_element_type=jnp.float32)
        loads[2 * i + 1].wait()
        hidden_grad = lax.dot_general(
            g_ref[...], downs[i], AGAINST_ROWS, preferred_element_type=jnp.float32
        )
        pre_grad = hidden_grad * silu_grad(pre_act)
        hidden[:, i * half : (i + 1) * half] = pre_grad.astype(jnp.bfloat16)
    me = lax.axis_index("expert")
    x, z, member = me // 32, (me // 4) % 8, (me % 4) // 2
    sources = [
        (x ^ (i // 2)) * 16 + ((z - k + 8) % 8) * 2 + (member ^ (i % 2))
        for batch in batches
        for i in range(4)
        for k in batch
    ]
    piece = groups // len(sources)
    for c in range(0, width, STEP):
        part = lax.dot_general(
            hidden[:, :half], ups[0, c : c + STEP, :], AGAINST_ROWS,
            preferred_element_type=jnp.float32,
        )
        part = part + lax.dot_general(
            hidden[:, half:], ups[1, c : c + STEP, :], AGAINST_ROWS,
            preferred_element_type=jnp.float32,
        )
        blocks = part.reshape(len(sources), piece, per_group, STEP).astype(jnp.bfloat16)
        for n, source in enumerate(sources):
            out_ref[pl.ds(source * piece, piece), :, c : c + STEP] = blocks[n]


def recipe_kernel(capacity, experts, info_ref, pick_ref, weight_ref):
    routes = info_ref[0:2, :].astype(jnp.int32)
    affinity = info_ref[2:4, :]
    tokens = routes.shape[1]
    rows = experts * capacity
    pick = slot_rows(place_of(routes, experts), capacity)
    row = lax.broadcasted_iota(jnp.int32, (rows, tokens), 0)
    weights = affinity / jnp.sum(affinity, 0, keepdims=True)
    for k in range(2):
        begin = routes[k : k + 1, :] * capacity
        mine = pick & (row >= begin) & (row < begin + capacity)
        pick_ref[k * tokens : (k + 1) * tokens, :] = as_bf16(mine).T
        weight_ref[k] = jnp.broadcast_to(weights[k : k + 1, :], (tokens, tokens)).T


def combine_kernel(pick_ref, weight_ref, x_ref, back_ref, out_ref):
    tokens = x_ref.shape[0]
    back = back_ref[...].reshape(pick_ref.shape[1], x_ref.shape[1])
    picked = jnp.dot(pick_ref[...], back, preferred_element_type=jnp.float32)
    total = x_ref[...].astype(jnp.float32)
    for k in range(2):
        total = total + weight_ref[k, :, 0:1] * picked[k * tokens : (k + 1) * tokens]
    out_ref[...] = total.astype(jnp.bfloat16)


def settle_kernel(in_ref, out_ref):
    out_ref[...] = in_ref[...]


def layer(
    x_fwd,
    routes_fwd,
    affinity_fwd,
    x_bwd,
    grad_bwd,
    routes_bwd,
    affinity_bwd,
    up_weight,
    down_weight,
):
    devices = lax.axis_size("expert")
    experts = devices // 2
    tokens = x_fwd.shape[1]
    model_width = x_fwd.shape[2]
    top_count = routes_fwd.shape[2]
    capacity = 3 * tokens * top_count // devices
    rows = experts * capacity
    groups = same_side_groups(devices)
    params = pltpu.CompilerParams(vmem_limit_bytes=63 * 1024 * 1024)

    up_own = up_weight[0]
    down_own = down_weight[0]
    up_other = from_partner(up_own, "expert")
    down_other = from_partner(down_own, "expert")

    routes_f = routes_fwd[0].T
    routes_b = routes_bwd[0].T

    def exchange(block):
        return lax.all_to_all(
            block, "expert", split_axis=0, concat_axis=0, tiled=True, axis_index_groups=groups
        )

    def dispatch(routes, blocks):
        count = len(blocks)
        groups_out = count * capacity // 4
        sent = pl.pallas_call(
            functools.partial(dispatch_kernel, capacity, experts, count),
            grid=(model_width // WIDE,),
            out_shape=jax.ShapeDtypeStruct((experts, groups_out, 4, model_width), jnp.bfloat16),
            in_specs=[pl.BlockSpec((top_count, tokens), lambda i: (0, 0))]
            + [pl.BlockSpec((tokens, WIDE), lambda i: (0, i))] * count,
            out_specs=pl.BlockSpec((experts, groups_out, 4, WIDE), lambda i: (0, 0, 0, i)),
            scratch_shapes=[pltpu.VMEM((rows, tokens), jnp.bfloat16)],
            compiler_params=params,
        )(routes, *blocks)
        return sent.reshape(experts * groups_out, 4, model_width)

    groups_b = 2 * capacity // 4
    sent_b = pl.pallas_call(
        functools.partial(dispatch_planes_kernel, capacity, experts),
        grid=(model_width // WIDE,),
        out_shape=[jax.ShapeDtypeStruct((4, groups_b, 4, model_width), jnp.bfloat16)] * 8,
        in_specs=[pl.BlockSpec((top_count, tokens), lambda i: (0, 0))]
        + [pl.BlockSpec((tokens, WIDE), lambda i: (0, i))] * 2,
        out_specs=[pl.BlockSpec((4, groups_b, 4, WIDE), lambda i: (0, 0, 0, i))] * 8,
        scratch_shapes=[pltpu.VMEM((rows, tokens), jnp.bfloat16)],
        compiler_params=params,
        name="dispatch_bwd",
    )(routes_b, x_bwd[0], grad_bwd[0])
    sent_b = [block.reshape(4 * groups_b, 4, model_width) for block in sent_b]

    def along_z(block, k):
        pairs = [(d, d // 32 * 32 + (d + 4 * k) % 32) for d in range(devices)]
        return lax.ppermute(block, "expert", pairs)

    def in_plane(block, i):
        pairs = [
            (d, (d ^ (32 * (i // 2))) // 4 * 4 + (3 - d % 4 if i % 2 else d % 4))
            for d in range(devices)
        ]
        return lax.ppermute(block, "expert", pairs)

    def regroup(blocks):
        count = len(blocks)
        return pl.pallas_call(
            functools.partial(regroup_kernel, groups_b),
            out_shape=[jax.ShapeDtypeStruct((count * groups_b, 4, model_width), jnp.bfloat16)] * 4,
            in_specs=[ANY] * count,
            out_specs=[ANY] * 4,
            scratch_shapes=[
                pltpu.VMEM((4, count * groups_b, 4, model_width), jnp.bfloat16),
                pltpu.SemaphoreType.DMA((4, count)),
                pltpu.SemaphoreType.DMA((4,)),
            ],
            compiler_params=params,
        )(*blocks)

    arrived = {k: along_z(sent_b[k], k) for batch in BATCHES for k in batch if k}
    arrived[0] = sent_b[0]
    recv_b = []
    for batch in BATCHES:
        by_member = regroup([arrived[k] for k in batch])
        recv_b += [in_plane(block, i) if i else block for i, block in enumerate(by_member)]
    recv_f = exchange(dispatch(routes_f, (x_fwd[0],)))

    half = up_own.shape[1]

    def serve(kernel, received, extra=()):
        return pl.pallas_call(
            kernel,
            out_shape=jax.ShapeDtypeStruct((rows // 4, 4, model_width), jnp.bfloat16),
            in_specs=[VMEM] * len(received) + [ANY] * 4,
            out_specs=VMEM,
            scratch_shapes=[
                pltpu.VMEM((2, model_width, half), jnp.bfloat16),
                pltpu.VMEM((2, half, model_width), jnp.bfloat16),
                pltpu.VMEM((rows, 2 * half), jnp.bfloat16),
                pltpu.SemaphoreType.DMA((4,)),
                *extra,
            ],
            compiler_params=params,
        )(*received, up_own, down_own, up_other, down_other)

    def recipe(info):
        return pl.pallas_call(
            functools.partial(recipe_kernel, capacity, experts),
            out_shape=(
                jax.ShapeDtypeStruct((top_count * tokens, rows), jnp.bfloat16),
                jax.ShapeDtypeStruct((top_count, tokens, tokens), jnp.float32),
            ),
            in_specs=[VMEM],
            out_specs=(VMEM, VMEM),
            compiler_params=params,
        )(info)

    def combine(pick_and_weight, x, back):
        return pl.pallas_call(
            combine_kernel,
            grid=(model_width // WIDE,),
            out_shape=jax.ShapeDtypeStruct((tokens, model_width), jnp.bfloat16),
            in_specs=[
                pl.BlockSpec((top_count * tokens, rows), lambda i: (0, 0)),
                pl.BlockSpec((top_count, tokens, tokens), lambda i: (0, 0, 0)),
                pl.BlockSpec((tokens, WIDE), lambda i: (0, i)),
                pl.BlockSpec((rows // 4, 4, WIDE), lambda i: (0, 0, i)),
            ],
            out_specs=pl.BlockSpec((tokens, WIDE), lambda i: (0, i)),
            compiler_params=params,
        )(*pick_and_weight, x, back)

    def settle(block):
        return pl.pallas_call(
            settle_kernel,
            out_shape=jax.ShapeDtypeStruct(block.shape, block.dtype),
            in_specs=[VMEM],
            out_specs=VMEM,
        )(block)

    def info_of(routes, affinity):
        return jnp.concatenate([routes.astype(jnp.float32), affinity[0].T], 0)

    served_b = serve(
        functools.partial(expert_bwd_kernel, BATCHES),
        recv_b,
        [pltpu.VMEM((rows, model_width), jnp.bfloat16)] * 2,
    )
    back_b = exchange(served_b)

    x_next = shifted(x_fwd[0], "section", 1)
    info_next = shifted(info_of(routes_f, affinity_fwd), "section", 1)
    served_f = serve(expert_fwd_kernel, [recv_f])
    served_f = shifted(served_f, "section", 1)
    back_f = exchange(served_f)

    recipe_b = recipe(info_of(routes_b, affinity_bwd))
    recipe_f = recipe(info_next)
    input_grad = combine(recipe_b, grad_bwd[0], back_b)
    bwd_next = shifted(input_grad, "section", -1)
    bwd_next = settle(bwd_next)
    fwd_next = combine(recipe_f, x_next, back_f)
    return (fwd_next[None], bwd_next[None])


def solution(mesh):
    rows = P("section", "expert", None)
    in_specs = (rows,) * 7 + (P("section", None, "expert"), rows)
    return jax.shard_map(
        layer, mesh=mesh, in_specs=in_specs, out_specs=(rows, rows), check_vma=False
    )
```
